64 devices in a mesh: rep: 4 (over x, y), dp: 16 (over z, core).
Axes of the slice: x: 2, y: 2, z: 8, core: 2. Of those that a mesh axis runs over, the one named last changes fastest.
The devices are a block of a 4x4x8 slice.
Arguments:
- x: bfloat16 [64, 1024, 640], P(('rep', 'dp')), parts along dimension 0
- dy: bfloat16 [64, 1024, 640], P(('rep', 'dp')), parts along dimension 0
- w_gate: bfloat16 [2, 640, 3456], P(None, 'dp')
- w_up: bfloat16 [2, 640, 3456], P(None, 'dp')
- w_down: bfloat16 [2, 3456, 640], P(None, 'dp')
- m_w_gate: float32 [2, 640, 3456], P(None, 'dp')
- m_w_up: float32 [2, 640, 3456], P(None, 'dp')
- m_w_down: float32 [2, 3456, 640], P(None, 'dp')
- v_w_gate: float32 [2, 640, 3456], P(None, 'dp')
- v_w_up: float32 [2, 640, 3456], P(None, 'dp')
- v_w_down: float32 [2, 3456, 640], P(None, 'dp')
Outputs:
- output 1: bfloat16 [8, 640, 3456], P('rep', 'dp'), parts along dimension 0
- output 2: bfloat16 [8, 640, 3456], P('rep', 'dp'), parts along dimension 0
- output 3: bfloat16 [8, 3456, 640], P('rep', 'dp'), parts along dimension 0
- output 4: float32 [8, 640, 3456], P('rep', 'dp'), parts along dimension 0
- output 5: float32 [8, 640, 3456], P('rep', 'dp'), parts along dimension 0
- output 6: float32 [8, 3456, 640], P('rep', 'dp'), parts along dimension 0
- output 7: float32 [8, 640, 3456], P('rep', 'dp'), parts along dimension 0
- output 8: float32 [8, 640, 3456], P('rep', 'dp'), parts along dimension 0
- output 9: float32 [8, 3456, 640], P('rep', 'dp'), parts along dimension 0
There are 4 independent parts. The reference program is written for one: setup_inputs(seed, part) draws one part's arguments, and reference() takes and returns one part's arrays. A program takes and returns all parts, laid end to end along the dimension named above; an argument that names none is the same for every part.
All inputs are finite; a program needn't handle non-finite values.
Results may differ from the reference program's by a relative error of at most 0.0224.
Values are sent between devices in bfloat16 or wider.
A program may use at most 768 MiB of HBM per device.

```python
import jax
import jax.numpy as jnp
from jax import lax

SEQUENCES = 16
TOKENS = 1024
D = 640
FF = 3456
LAYERS = 2
NAMES = ("w_gate", "w_up", "w_down")
SHAPES = {"w_gate": (LAYERS, D, FF), "w_up": (LAYERS, D, FF), "w_down": (LAYERS, FF, D)}


def bump(key, n, height):
    away = (jnp.arange(n, dtype=jnp.int32) - jax.random.randint(key, (), 0, n, jnp.int32)) % n
    return jnp.where(away < n // 8, height, 1.0)


def together(key, own, strength):
    shared = jax.random.normal(key, own.shape[1:], jnp.float32)
    return (own + strength * shared) * lax.rsqrt(1 + strength * strength)


def setup_inputs(seed: int = 0, part: int = 0) -> dict:
    kx, kdy, ka, kb, kz, kf, kh, kl, *keys = jax.random.split(jax.random.key(seed), 8 + 3 * len(NAMES))
    kx, kdy, ka, kb = (jax.random.fold_in(k, part) for k in (kx, kdy, ka, kb))
    kw, km, kv = (keys[i::3] for i in range(3))
    shape = (SEQUENCES, TOKENS, D)
    much_x, much_dy = jax.random.uniform(kz, (2,), jnp.float32, 0.0, 1.0)
    loud = 2.0 ** jax.random.uniform(jax.random.fold_in(kz, 1), (), jnp.float32, -1.0, 2.0)
    layers = 2.0 ** jax.random.uniform(kl, (LAYERS, 1, 1), jnp.float32, -1.0, 1.0)
    x = together(ka, jax.random.normal(kx, shape, jnp.float32), much_x) * bump(kf, D, 4.0)
    dy = together(kb, jax.random.normal(kdy, shape, jnp.float32), much_dy)
    drawn = {"x": x.astype(jnp.bfloat16), "dy": (loud * dy * (SEQUENCES * TOKENS) ** -0.5).astype(jnp.bfloat16)}
    for key, name in zip(kw, NAMES, strict=True):
        w = jax.random.normal(key, SHAPES[name], jnp.float32) * SHAPES[name][1] ** -0.5
        drawn[name] = (w * {"w_gate": 1.0, "w_up": bump(kh, FF, 4.0), "w_down": layers}[name]).astype(jnp.bfloat16)
    for key, name in zip(km, NAMES, strict=True):
        drawn[f"m_{name}"] = 0.1 * jax.random.normal(key, SHAPES[name], jnp.float32)
    for key, name in zip(kv, NAMES, strict=True):
        drawn[f"v_{name}"] = jax.random.uniform(key, SHAPES[name], jnp.float32, 0.005, 0.015)
    return drawn


def matmul(a, w):
    return jnp.dot(a, w, preferred_element_type=jnp.float32).astype(jnp.bfloat16)


def normed(h):
    wide = h.astype(jnp.float32)
    scale = lax.rsqrt(jnp.mean(wide**2, -1, keepdims=True) + 1e-6)
    return (wide * scale).astype(jnp.bfloat16)


def layer(h, w):
    a = normed(h)
    gate = jnp.dot(a, w["w_gate"], preferred_element_type=jnp.float32)
    up = jnp.dot(a, w["w_up"], preferred_element_type=jnp.float32)
    return h + matmul((jax.nn.silu(gate) * up).astype(jnp.bfloat16), w["w_down"])


def adamw(w, m, v, g):
    m = 0.9 * m + 0.1 * g
    v = 0.95 * v + 0.05 * g * g
    step = m * lax.rsqrt(v + 1e-8) + 0.1 * w
    return (w - 0.02 * step).astype(jnp.bfloat16), m, v


def clipped(gradients, sum_of_squares, count):
    factor = jnp.minimum(1.0, 0.5 * lax.rsqrt(sum_of_squares / count + 1e-30))
    return [g * factor for g in gradients]


def stack(weights, h):
    return lax.scan(lambda h, w: (layer(h, w), None), h, weights)[0]


def reference(x, dy, w_gate, w_up, w_down, m_w_gate, m_w_up, m_w_down, v_w_gate, v_w_up, v_w_down):
    weights = dict(zip(NAMES, (w_gate, w_up, w_down), strict=True))

    def take(so_far, sequence):
        h, by_y = sequence
        _, back = jax.vjp(lambda w: stack(w, h), weights)
        return jax.tree.map(lambda total, term: total + term.astype(jnp.float32), so_far, back(by_y)[0]), None

    none_yet = {name: jnp.zeros(w.shape, jnp.float32) for name, w in weights.items()}
    by_weights, _ = lax.scan(take, none_yet, (x, dy))
    gradients = [by_weights[name].astype(jnp.bfloat16).astype(jnp.float32) for name in NAMES]
    gradients = clipped(gradients, sum(jnp.sum(g * g) for g in gradients), sum(g.size for g in gradients))
    new = [
        adamw(w.astype(jnp.float32), m, v, g)
        for w, m, v, g in zip((w_gate, w_up, w_down), (m_w_gate, m_w_up, m_w_down), (v_w_gate, v_w_up, v_w_down), gradients, strict=True)
    ]
    return tuple(one[which] for which in range(3) for one in new)
```

```python
import functools

import jax
import jax.numpy as jnp
from jax import lax
from jax.experimental import pallas as pl
from jax.experimental.pallas import tpu as pltpu
from jax.sharding import PartitionSpec as P

MESH = pl.DeviceIdType.MESH
ANY = pl.BlockSpec(memory_space=pltpu.HBM)
F32, BF16 = jnp.float32, jnp.bfloat16
SK = 2
SLOTS = 8
GSLOTS = 16
RSLOTS = 8
DCH = 3
CHUNKS = 9
PIECES = 9


def mm(a, b):
    return jnp.dot(a, b, preferred_element_type=F32)


def mm_nt(a, b):
    return lax.dot_general(a, b, (((1,), (1,)), ((), ())), preferred_element_type=F32)


def mm_tn(a, b):
    return lax.dot_general(a, b, (((0,), (0,)), ((), ())), preferred_element_type=F32)


def train_kernel(nz, x, dy, wg, wu, wd, ggu, gd, sqo, WGU, WD,
                 H, DY, A, AT, DACC, WC, WDC, DGU, ACT, TS, R, TD, RD, BG, BD, FG, FD, SQ, SQALL, sgu, sd,
                 load_sem, w_sem, own_sem, g_recv, g_sib, g_send,
                 r_send, r_recv, ring_send, ring_recv, fin_send, fin_recv, sq_send, sq_recv):
    me = lax.axis_index("dp")
    z, c = me // 2, me % 2
    n = 2 * nz
    half = nz // 2
    tokens, d = H.shape
    rgu = d // n
    cw = TS.shape[-1]
    ff = cw * CHUNKS
    rd = ff // n
    drow = rd // DCH
    crd = 2 * rd
    prow = crd // PIECES
    items = (PIECES + 1) // 2
    per = CHUNKS + items
    total = 2 * per
    gper = DCH + CHUNKS
    gtotal = 2 * gper
    gdone = SK * half + 2
    UF = DCH + gdone + 1
    U1 = gper + DCH + gdone + 1
    U2 = U1 + CHUNKS + 1

    def dev(zz, cc):
        return {"dp": lax.rem(zz + nz, nz) * 2 + cc}

    def remote(src, dst, s, r, to):
        return pltpu.make_async_remote_copy(src, dst, s, r, device_id=to, device_id_type=MESH)

    def wait(ref, sem):
        remote(ref, ref, sem, sem, dev(z, 1 - c)).wait_recv()

    first = [pltpu.make_async_copy(x, H, load_sem.at[0]), pltpu.make_async_copy(dy, DY, load_sem.at[1]), pltpu.make_async_copy(wd, sd, load_sem.at[2])]
    for cp in first:
        cp.start()
    for j in range(CHUNKS):
        for m, w in enumerate((wg, wu)):
            pltpu.make_async_copy(w.at[:, :, j * cw : (j + 1) * cw], sgu.at[:, :, (2 * j + m) * cw : (2 * j + m + 1) * cw], load_sem.at[3]).start()

    barrier = pltpu.get_barrier_semaphore()
    for i in range(1, n):
        pl.semaphore_signal(barrier, inc=1, device_id={"dp": lax.rem(me + i, n)}, device_id_type=MESH)
    pl.semaphore_wait(barrier, n - 1)
    for cp in first:
        cp.wait()
    pltpu.make_async_copy(WGU.at[:, :rgu, :], sgu, load_sem.at[3]).wait()

    SQ[...] = jnp.zeros_like(SQ)

    def normalize(src, transposed):
        def rows(i, _):
            rs = pl.ds(pl.multiple_of(i * 128, 128), 128)
            wide = src[rs, :].astype(F32)
            a = (wide * lax.rsqrt(jnp.mean(wide * wide, -1, keepdims=True) + 1e-6)).astype(BF16)
            A[rs, :] = a
            if transposed:
                AT[:, rs] = a.T
            return 0
        lax.fori_loop(0, tokens // 128, rows, 0)

    def piece(q, src_z, own, fn):
        layer, r = q // gper, q % gper
        blk = lax.rem(src_z + nz, nz) * 2 + c
        @pl.when(r < DCH)
        def _():
            dst = WD.at[layer, pl.ds(pl.multiple_of(blk * rd + r * drow, 8), drow), :]
            fn(sd.at[layer, pl.ds(pl.multiple_of(r * drow, 8), drow), :] if own else dst, dst)
        @pl.when(r >= DCH)
        def _():
            cs = pl.ds(pl.multiple_of((r - DCH) * 2 * cw, 128), 2 * cw)
            dst = WGU.at[layer, pl.ds(pl.multiple_of(blk * rgu, 8), rgu), cs]
            fn(sgu.at[layer, :, cs] if own else dst, dst)

    def to_sibling(q, src, dst):
        remote(src, dst, g_send.at[q % GSLOTS], g_sib.at[q % GSLOTS], dev(z, 1 - c)).start()

    def to_next(q, way, hop, src, dst):
        to = z + 1 if way == 0 else z - 1
        remote(src, dst, g_send.at[q % GSLOTS], g_recv.at[way, hop - 1, q % RSLOTS], dev(to, c)).start()

    def gather_step(t):
        @pl.when(t < gtotal)
        def _():
            def own(src, dst):
                to_next(t, 0, 1, src, dst)
                to_next(t, 1, 1, src, dst)
                to_sibling(t, src, dst)
                pltpu.make_async_copy(src, dst, own_sem.at[t % GSLOTS]).start()
            piece(t, z, True, own)
        for h in range(1, half + 1):
            q = t - SK * h
            for way in (0, 1):
                longer = q % 2 == way
                ok = (q >= 0) & (q < gtotal)
                if h == half:
                    ok = ok & longer
                @pl.when(ok)
                def _():
                    def go(src, dst):
                        remote(src, dst, g_send.at[0], g_recv.at[way, h - 1, q % RSLOTS], dev(z, 1 - c)).wait_recv()
                        if h < half - 1:
                            to_next(q, way, h + 1, src, dst)
                        elif h == half - 1:
                            @pl.when(longer)
                            def _():
                                to_next(q, way, h + 1, src, dst)
                        to_sibling(q, src, dst)
                    piece(q, z - h if way == 0 else z + h, False, go)
        q = t - gdone
        @pl.when((q >= 0) & (q < gtotal))
        def _():
            layer, r, slot = q // gper, q % gper, q % GSLOTS
            def both(ref):
                for rows, sem in ((1, own_sem), (nz, g_sib), (2 * nz - 1, g_send)):
                    a = ref(rows)
                    pltpu.make_async_copy(a, a, sem.at[slot]).wait()
            @pl.when(r < DCH)
            def _():
                both(lambda k: WD.at[layer, pl.ds(0, k * drow), :])
            @pl.when(r >= DCH)
            def _():
                cs = pl.ds(pl.multiple_of((r - DCH) * 2 * cw, 128), 2 * cw)
                both(lambda k: WGU.at[layer, pl.ds(0, k * rgu), cs])

    def work(u):
        k0, k1, k2 = u - UF, u - U1, u - U2
        on = lambda k: (k >= 0) & (k < CHUNKS)
        kind = jnp.where(u < U1, 0, jnp.where(u < U2, 1, 2))
        return on(k0) | on(k1) | on(k2), kind, jnp.where(u < U1, k0, jnp.where(u < U2, k1, k2))

    def weights(u):
        on, kind, j = work(u)
        layer = jnp.where(kind == 1, 1, 0)
        slot = u % 2
        return on, (pltpu.make_async_copy(WGU.at[layer, :, pl.ds(pl.multiple_of(j * 2 * cw, 128), 2 * cw)], WC.at[slot], w_sem.at[slot, 0]),
                    pltpu.make_async_copy(WD.at[layer, pl.ds(pl.multiple_of(j * cw, 128), cw), :], WDC.at[slot], w_sem.at[slot, 1]))

    def forward(j, slot):
        gu = mm(A[...], WC[slot])
        g, up = gu[:, :cw], gu[:, cw:]
        ACT[...] = (g * jax.nn.sigmoid(g) * up).astype(BF16)
        @pl.when(j == 0)
        def _():
            DACC[...] = jnp.zeros_like(DACC)
        DACC[...] += mm(ACT[...], WDC[slot])

    def compute(j, slot):
        gu = mm(A[...], WC[slot])
        g, up = gu[:, :cw], gu[:, cw:]
        back = mm_nt(DY[...], WDC[slot]).astype(BF16).astype(F32)
        sg = jax.nn.sigmoid(g)
        s = g * sg
        ACT[...] = (s * up).astype(BF16)
        DGU[:, :cw] = (back * up * (sg + s * (1.0 - sg))).astype(BF16)
        DGU[:, cw:] = (back * s).astype(BF16)
        t = mm(AT[...], DGU[...]).astype(BF16)
        TS[0, j] = t[:, :cw]
        TS[1, j] = t[:, cw:]

    def compute_rest(kind, j, slot):
        @pl.when(kind == 1)
        def _():
            @pl.when(j == 0)
            def _():
                DACC[...] = jnp.zeros_like(DACC)
            DACC[...] += mm_nt(DGU[...], WC[slot])
        TD[jnp.where(kind == 1, 1, 0), pl.ds(pl.multiple_of(j * cw, 128), cw), :] = mm_tn(ACT[...], DY[...]).astype(BF16)

    def after_forward():
        def rows(i, _):
            rs = pl.ds(pl.multiple_of(i * 128, 128), 128)
            H[rs, :] = (H[rs, :].astype(F32) + DACC[rs, :].astype(BF16).astype(F32)).astype(BF16)
            return 0
        lax.fori_loop(0, tokens // 128, rows, 0)
        normalize(H, True)

    def between():
        xin = pltpu.make_async_copy(x, A, load_sem.at[0])
        xin.start()
        def rows(i, _):
            rs = pl.ds(pl.multiple_of(i * 128, 128), 128)
            wide = H[rs, :].astype(F32)
            scale = lax.rsqrt(jnp.mean(wide * wide, -1, keepdims=True) + 1e-6)
            da = DACC[rs, :].astype(BF16).astype(F32)
            dh = scale * da - wide * (scale * scale * scale * jnp.mean(wide * da, -1, keepdims=True))
            DY[rs, :] = (DY[rs, :].astype(F32) + dh.astype(BF16).astype(F32)).astype(BF16)
            return 0
        lax.fori_loop(0, tokens // 128, rows, 0)
        xin.wait()
        normalize(A, True)

    def item(i):
        return 1 - i // per, i % per

    def piece_of(layer, k, cc):
        return 2 * k + lax.rem(cc + layer, 2)

    def send_terms(i, start):
        layer, r = item(i)
        @pl.when(r < CHUNKS)
        def _():
            cp = remote(TS.at[1 - c, r], R.at[r], r_send, r_recv.at[i], dev(z, 1 - c))
            cp.start() if start else cp.wait_send()
        @pl.when(r >= CHUNKS)
        def _():
            k = r - CHUNKS
            p = piece_of(layer, k, 1 - c)
            @pl.when(p < PIECES)
            def _():
                if start:
                    for zz in range(nz):
                        rs = pl.ds(pl.multiple_of(zz * crd + p * prow, 16), prow)
                        remote(TD.at[layer, rs, :], RD.at[k, zz], r_send, r_recv.at[i], dev(z, 1 - c)).start()
                else:
                    wait(RD.at[k], r_send)

    def terms(i, zz, fn):
        layer, r = item(i)
        zz = lax.rem(zz + 2 * nz, nz)
        @pl.when(r < CHUNKS)
        def _():
            rs = pl.ds(pl.multiple_of(zz * 2 * rgu, 16), 2 * rgu)
            fn(TS.at[c, r, rs, :], R.at[r, rs, :], BG, r % 2, True)
        @pl.when(r >= CHUNKS)
        def _():
            k = r - CHUNKS
            p = piece_of(layer, k, c)
            @pl.when(p < PIECES)
            def _():
                fn(TD.at[layer, pl.ds(pl.multiple_of(zz * crd + p * prow, 16), prow), :], RD.at[k, zz], BD, k % 2, False)

    def ring_copy(i, way, s, buf):
        to = z + 1 if way == 0 else z - 1
        slot = i % SLOTS
        return remote(buf.at[way, s, slot], buf.at[way, s + 1, slot], ring_send.at[way, s, slot], ring_recv.at[way, s, slot], dev(to, c))

    def arrived(i, way, s, buf):
        slot = i % SLOTS
        wait(buf.at[way, s, slot], ring_recv.at[way, s - 1, slot])

    def stage(i, way, s):
        def fn_for(hops):
            def fn(own, other, buf, odd, is_gu):
                mine = (odd == way) if hops == half else (odd != way)
                @pl.when(mine)
                def _():
                    slot = i % SLOTS
                    t = own[...].astype(F32) + other[...].astype(F32)
                    if s > 0:
                        arrived(i, way, s, buf)
                        t = t + buf[way, s, slot].astype(F32)
                    buf[way, s, slot] = t.astype(BF16)
                    ring_copy(i, way, s, buf).start()
            return fn
        for hops in (half, half - 1):
            if s < hops:
                terms(i, z + (hops - s) if way == 0 else z - (hops - s), fn_for(hops))

    def stage_sent(i, way, s):
        def fn(own, other, buf, odd, is_gu):
            def go():
                ring_copy(i, way, s, buf).wait_send()
            if s < half - 1:
                go()
            else:
                pl.when(odd == way)(go)
        terms(i, z, fn)

    def last(i):
        layer, r = item(i)
        slot = i % SLOTS
        def fn(own, other, buf, odd, is_gu):
            def add(hops_up):
                t = own[...].astype(F32) + other[...].astype(F32)
                for way, hops in ((0, hops_up), (1, nz - 1 - hops_up)):
                    arrived(i, way, hops, buf)
                    t = t + buf[way, hops, slot].astype(F32)
                w = t.astype(BF16).astype(F32)
                sq = SQ[...]
                for a in range(w.shape[0] // 8):
                    for b in range(w.shape[1] // 128):
                        v = w[8 * a : 8 * a + 8, 128 * b : 128 * b + 128]
                        sq = sq + v * v
                SQ[...] = sq
                out, rows = (FG, rgu) if is_gu else (FD, prow // 2)
                out[slot, 0] = w[:rows].astype(BF16)
                out[slot, 1] = w[rows:].astype(BF16)
            @pl.when(odd == 0)
            def _():
                add(half)
            @pl.when(odd == 1)
            def _():
                add(half - 1)
            if is_gu:
                cs = pl.ds(pl.multiple_of(r * cw, 128), cw)
                pltpu.make_async_copy(FG.at[slot, c], ggu.at[layer, c, :, cs], fin_send.at[0, slot]).start()
                remote(FG.at[slot, 1 - c], ggu.at[layer, c, :, cs], fin_send.at[1, slot], fin_recv.at[layer, 0], dev(z, 1 - c)).start()
            else:
                p = piece_of(layer, r - CHUNKS, c)
                for b in range(2):
                    k = 2 * p + b
                    dst = gd.at[layer, pl.ds(pl.multiple_of(lax.rem(k, PIECES) * (prow // 2), 8), prow // 2), :]
                    @pl.when(k // PIECES == c)
                    def _():
                        pltpu.make_async_copy(FD.at[slot, b], dst, fin_send.at[b, slot]).start()
                    @pl.when(k // PIECES != c)
                    def _():
                        remote(FD.at[slot, b], dst, fin_send.at[b, slot], fin_recv.at[layer, 1], dev(z, 1 - c)).start()
        terms(i, z, fn)

    def last_sent(i):
        slot = i % SLOTS
        def fn(own, other, buf, odd, is_gu):
            for b in range(2):
                wait((FG if is_gu else FD).at[slot, b], fin_send.at[b, slot])
        terms(i, z, fn)

    def valid(i):
        return (i >= 0) & (i < total)

    def reduce_step(t):
        @pl.when(valid(t - 1))
        def _():
            send_terms(t - 1, False)
        for s in range(half):
            i = t - 2 - SK * s
            @pl.when(valid(i))
            def _():
                for way in (0, 1):
                    stage_sent(i, way, s)
        before = t - 2 - SK * half
        @pl.when(valid(before))
        def _():
            last_sent(before)
        final = t - 1 - SK * half
        @pl.when(valid(final))
        def _():
            last(final)
        for s in reversed(range(half)):
            i = t - 1 - SK * s
            @pl.when(valid(i))
            def _():
                if s == 0:
                    layer, r = item(i)
                    @pl.when(r < CHUNKS)
                    def _():
                        wait(R.at[r], r_recv.at[i])
                    @pl.when((r >= CHUNKS) & (piece_of(layer, r - CHUNKS, c) < PIECES))
                    def _():
                        wait(RD.at[r - CHUNKS], r_recv.at[i])
                for way in (0, 1):
                    stage(i, way, s)

    normalize(H, False)

    def step(u, _):
        t = u - U1
        @pl.when(u < gtotal + gdone)
        def _():
            gather_step(u)
        @pl.when(t >= 0)
        def _():
            reduce_step(t)

        on, kind, j = work(u)
        slot = u % 2
        following, loads = weights(u + 1)
        @pl.when(following)
        def _():
            for cp in loads:
                cp.start()
        @pl.when(u == U1 - 1)
        def _():
            after_forward()
        @pl.when(u == U2 - 1)
        def _():
            between()
        @pl.when(on)
        def _():
            for cp in weights(u)[1]:
                cp.wait()
        @pl.when(on & (kind == 0))
        def _():
            forward(j, slot)
        @pl.when(on & (kind > 0))
        def _():
            compute(j, slot)
        @pl.when(valid(t))
        def _():
            send_terms(t, True)
        @pl.when(on & (kind > 0))
        def _():
            compute_rest(kind, j, slot)
        return 0

    lax.fori_loop(0, U1 + total + SK * half + 2, step, 0)

    for i in range(1, n):
        remote(SQ, SQALL.at[me], sq_send, sq_recv, {"dp": lax.rem(me + i, n)}).start()
    for layer in range(2):
        wait(ggu.at[layer, 0], fin_recv.at[layer, 0])
        even = lax.rem(c + layer, 2) == 0
        @pl.when(even)
        def _():
            wait(gd.at[layer, pl.ds(0, PIECES // 2 * (prow // 2)), :], fin_recv.at[layer, 1])
        @pl.when(jnp.logical_not(even))
        def _():
            wait(gd.at[layer, pl.ds(0, (PIECES + 1) // 2 * (prow // 2)), :], fin_recv.at[layer, 1])
    wait(SQALL.at[pl.ds(0, n - 1)], sq_recv)
    acc = SQ[...]
    for i in range(1, n):
        acc = acc + SQALL[lax.rem(me + i, n)]
    sqo[...] = acc
    wait(SQALL.at[pl.ds(0, n - 1)], sq_send)


def train(mesh, x, dy, w_gate, w_up, w_down):
    n = mesh.shape["dp"]
    nz = n // 2
    half = nz // 2
    tokens, d = x.shape
    layers, rgu, ff = w_gate.shape
    rd = ff // n
    cw = ff // CHUNKS
    prow = 2 * rd // PIECES
    items = (PIECES + 1) // 2
    total = 2 * (CHUNKS + items)
    V, S = pltpu.VMEM, pltpu.SemaphoreType.DMA
    shape = jax.ShapeDtypeStruct
    return pl.pallas_call(
        functools.partial(train_kernel, nz),
        out_shape=(
            shape((layers, 2, rgu, ff), BF16), shape((layers, rd, d), BF16), shape((8, 128), F32),
            shape((layers, d, 2 * ff), BF16), shape((layers, ff, d), BF16),
        ),
        in_specs=[ANY] * 5,
        out_specs=(ANY, ANY, pl.BlockSpec(memory_space=pltpu.VMEM), ANY, ANY),
        scratch_shapes=[
            V((tokens, d), BF16), V((tokens, d), BF16), V((tokens, d), BF16), V((d, tokens), BF16), V((tokens, d), F32),
            V((2, d, 2 * cw), BF16), V((2, cw, d), BF16), V((tokens, 2 * cw), BF16), V((tokens, cw), BF16),
            V((2, CHUNKS, d, cw), BF16), V((CHUNKS, d, cw), BF16), V((layers, ff, d), BF16), V((items, nz, prow, d), BF16),
            V((2, half + 1, SLOTS, 2 * rgu, cw), BF16), V((2, half + 1, SLOTS, prow, d), BF16),
            V((SLOTS, 2, rgu, cw), BF16), V((SLOTS, 2, prow // 2, d), BF16),
            V((8, 128), F32), V((n, 8, 128), F32), V((layers, rgu, 2 * ff), BF16), V((layers, rd, d), BF16),
            S((4,)), S((2, 2)), S((GSLOTS,)), S((2, half, RSLOTS)), S((GSLOTS,)), S((GSLOTS,)),
            S, S((total,)), S((2, half, SLOTS)), S((2, half, SLOTS)), S((2, SLOTS)), S((layers, 2)), S, S,
        ],
        compiler_params=pltpu.CompilerParams(collective_id=0, has_side_effects=True, vmem_limit_bytes=63 * 2**20),
        name="train",
    )(x, dy, w_gate, w_up, w_down)


def adamw(w, m, v, g):
    m = 0.9 * m + 0.1 * g
    v = 0.95 * v + 0.05 * g * g
    step = m * lax.rsqrt(v + 1e-8) + 0.1 * w
    return (w - 0.02 * step).astype(BF16), m, v


def solution(mesh):
    n = mesh.shape["dp"]

    def step(x, dy, *arrays):
        weights, m, v = (arrays[i : i + 3] for i in (0, 3, 6))
        ggu, gd, squares = train(mesh, x[0], dy[0], *weights)[:3]
        gradients = [g.astype(F32) for g in (ggu[:, 0], ggu[:, 1], gd)]
        count = n * sum(g.size for g in gradients)
        factor = jnp.minimum(1.0, 0.5 * lax.rsqrt(jnp.sum(squares) / count + 1e-30))
        new = [adamw(w.astype(F32), m, v, g * factor) for w, m, v, g in zip(weights, m, v, gradients, strict=True)]
        return tuple(one[which] for which in range(3) for one in new)

    states, cut = P(("rep", "dp"), None, None), P(None, "dp", None)
    return jax.shard_map(
        step,
        mesh=mesh,
        in_specs=(states, states) + (cut,) * 9,
        out_specs=(P("rep", "dp", None),) * 9,
        check_vma=False,
    )
```

```python
import functools
import math

import jax
import jax.numpy as jnp
from jax import lax
from jax.experimental import pallas as pl
from jax.experimental.pallas import tpu as pltpu
from jax.sharding import PartitionSpec as P

MESH = pl.DeviceIdType.MESH
ANY = pl.BlockSpec(memory_space=pltpu.HBM)
F32, BF16 = jnp.float32, jnp.bfloat16
SK = 2
SLOTS = 8
GSLOTS = 16
RSLOTS = 8
GPAR = 2
DCH = 3
CHUNKS = 9
PIECES = 9


def mm(a, b):
    return jnp.dot(a, b, preferred_element_type=F32)


def mm_nt(a, b):
    return lax.dot_general(a, b, (((1,), (1,)), ((), ())), preferred_element_type=F32)


def mm_tn(a, b):
    return lax.dot_general(a, b, (((0,), (0,)), ((), ())), preferred_element_type=F32)


def train_kernel(nz, ny, x, dy, wg, wu, wd, ggu, gd, sqo, WGU, WD,
                 H, DY, A, AT, DACC, WC, WDC, DGU, ACT, TS, R, TD, RD, BG, BD, FG, FD, SQ, SQALL, sgu, sd,
                 load_sem, w_sem, own_sem, g_recv, g_sib, g_send, g_par,
                 r_send, r_recv, ring_send, ring_recv, fin_send, fin_recv, sq_send, sq_recv):
    me = lax.axis_index("dp")
    z, c = me // 2, me % 2
    n = 2 * nz
    half = nz // 2
    tokens, d = H.shape
    rgu = d // n
    cw = TS.shape[-1]
    ff = cw * CHUNKS
    rd = ff // n
    drow = rd // DCH
    crd = 2 * rd
    prow = crd // PIECES
    items = (PIECES + 1) // 2
    per = CHUNKS + items
    total = 2 * per
    gper = DCH + CHUNKS
    gtotal = 2 * gper
    dhalf = (drow // 16 + 1) * 8
    gpar = SK * half + GPAR
    gdone = gpar + 1
    UF = DCH + gdone + 1
    U1 = gper + DCH + gdone + 1
    U2 = U1 + CHUNKS + 1

    rep = lax.axis_index("rep")
    gx, gy = rep // ny, rep % ny
    diagonal = lax.rem(gx + gy, 2)
    beside_y = rep + 1 - 2 * lax.rem(gy, 2)
    beside_x = rep + ny * (1 - 2 * lax.rem(gx, 2))

    def dev(zz, cc):
        return {"dp": lax.rem(zz + nz, nz) * 2 + cc}

    def remote(src, dst, s, r, to):
        return pltpu.make_async_remote_copy(src, dst, s, r, device_id=to, device_id_type=MESH)

    def wait(ref, sem):
        remote(ref, ref, sem, sem, dev(z, 1 - c)).wait_recv()

    first = [pltpu.make_async_copy(x, H, load_sem.at[0]), pltpu.make_async_copy(dy, DY, load_sem.at[1]), pltpu.make_async_copy(wd, sd, load_sem.at[2])]
    for cp in first:
        cp.start()
    for j in range(CHUNKS):
        for m, w in enumerate((wg, wu)):
            pltpu.make_async_copy(w.at[:, :, j * cw : (j + 1) * cw], sgu.at[:, :, (2 * j + m) * cw : (2 * j + m + 1) * cw], load_sem.at[3]).start()

    barrier = pltpu.get_barrier_semaphore()
    for i in range(1, n):
        pl.semaphore_signal(barrier, inc=1, device_id={"dp": lax.rem(me + i, n)}, device_id_type=MESH)
    for to in (beside_x, beside_y):
        pl.semaphore_signal(barrier, inc=1, device_id={"rep": to, "dp": me}, device_id_type=MESH)
    pl.semaphore_wait(barrier, n + 1)
    for cp in first:
        cp.wait()
    pltpu.make_async_copy(WGU.at[:, :rgu, :], sgu, load_sem.at[3]).wait()

    SQ[...] = jnp.zeros_like(SQ)

    def normalize(src, transposed):
        def rows(i, _):
            rs = pl.ds(pl.multiple_of(i * 128, 128), 128)
            wide = src[rs, :].astype(F32)
            a = (wide * lax.rsqrt(jnp.mean(wide * wide, -1, keepdims=True) + 1e-6)).astype(BF16)
            A[rs, :] = a
            if transposed:
                AT[:, rs] = a.T
            return 0
        lax.fori_loop(0, tokens // 128, rows, 0)

    def piece(q, blk, part, own, fn):
        layer, r = q // gper, q % gper
        @pl.when(r < DCH)
        def _():
            def rows(first, size):
                here = pl.ds(pl.multiple_of(r * drow + first, 8), size)
                dst = WD.at[layer, pl.ds(pl.multiple_of(blk * rd + r * drow + first, 8), size), :]
                fn(sd.at[layer, here, :] if own else dst, dst)
            if part == 2:
                rows(0, drow)
            else:
                @pl.when(diagonal == part)
                def _():
                    rows(0, dhalf)
                @pl.when(diagonal != part)
                def _():
                    rows(dhalf, drow - dhalf)
        @pl.when(r >= DCH)
        def _():
            start, size = (r - DCH) * 2 * cw, 2 * cw
            if part < 2:
                start, size = start + lax.rem(diagonal + part, 2) * cw, cw
            cs = pl.ds(pl.multiple_of(start, 128), size)
            dst = WGU.at[layer, pl.ds(pl.multiple_of(blk * rgu, 8), rgu), cs]
            fn(sgu.at[layer, :, cs] if own else dst, dst)

    def block(zz):
        return lax.rem(zz + nz, nz) * 2 + c

    def to_sibling(q, src, dst):
        remote(src, dst, g_send.at[q % GSLOTS], g_sib.at[q % GSLOTS], dev(z, 1 - c)).start()

    def to_next(q, way, hop, src, dst):
        to = z + 1 if way == 0 else z - 1
        remote(src, dst, g_send.at[q % GSLOTS], g_recv.at[way, hop - 1, q % RSLOTS], dev(to, c)).start()

    def to_beside(q, src, dst):
        to = jnp.where(q % 2 == 0, beside_y, beside_x)
        remote(src, dst, g_send.at[q % GSLOTS], g_par.at[q % GSLOTS], {"rep": to, "dp": me}).start()

    def gather_step(t):
        @pl.when(t < gtotal)
        def _():
            def own(src, dst):
                to_next(t, 0, 1, src, dst)
                to_next(t, 1, 1, src, dst)
            piece(t, me, 0, True, own)
            def whole(src, dst):
                to_sibling(t, src, dst)
                pltpu.make_async_copy(src, dst, own_sem.at[t % GSLOTS]).start()
            piece(t, me, 2, True, whole)
        for h in range(1, half + 1):
            q = t - SK * h
            for way in (0, 1):
                longer = q % 2 == way
                ok = (q >= 0) & (q < gtotal)
                if h == half:
                    ok = ok & longer
                @pl.when(ok)
                def _():
                    def go(src, dst):
                        remote(src, dst, g_send.at[0], g_recv.at[way, h - 1, q % RSLOTS], dev(z, 1 - c)).wait_recv()
                        if h < half - 1:
                            to_next(q, way, h + 1, src, dst)
                        elif h == half - 1:
                            @pl.when(longer)
                            def _():
                                to_next(q, way, h + 1, src, dst)
                        to_beside(q, src, dst)
                        to_sibling(q, src, dst)
                    piece(q, block(z - h if way == 0 else z + h), 0, False, go)
        q = t - gpar
        @pl.when((q >= 0) & (q < gtotal))
        def _():
            layer, r, slot = q // gper, q % gper, q % GSLOTS
            @pl.when(r < DCH)
            def _():
                for theirs in range(2):
                    @pl.when(diagonal != theirs)
                    def _():
                        wait(WD.at[layer, pl.ds(0, (nz - 1) * (drow - dhalf if theirs else dhalf)), :], g_par.at[slot])
            @pl.when(r >= DCH)
            def _():
                wait(WGU.at[layer, pl.ds(0, (nz - 1) * rgu), pl.ds(0, cw)], g_par.at[slot])
            for h in range(1, nz):
                piece(q, block(z + h), 1, False, lambda src, dst: to_sibling(q, src, dst))
        q = t - gdone
        @pl.when((q >= 0) & (q < gtotal))
        def _():
            layer, r, slot = q // gper, q % gper, q % GSLOTS
            def waited(ref, sem):
                pltpu.make_async_copy(ref, ref, sem.at[slot]).wait()
            @pl.when(r < DCH)
            def _():
                rows = lambda k: WD.at[layer, pl.ds(0, k), :]
                waited(rows(drow), own_sem)
                waited(rows(nz * drow), g_sib)
                for mine in range(2):
                    @pl.when(diagonal == mine)
                    def _():
                        waited(rows(nz * drow + 2 * (nz - 1) * (drow - dhalf if mine else dhalf)), g_send)
            @pl.when(r >= DCH)
            def _():
                cs = pl.ds(pl.multiple_of((r - DCH) * 2 * cw, 128), 2 * cw)
                for k, sem in ((1, own_sem), (nz, g_sib), (2 * nz - 1, g_send)):
                    waited(WGU.at[layer, pl.ds(0, k * rgu), cs], sem)

    def work(u):
        k0, k1, k2 = u - UF, u - U1, u - U2
        on = lambda k: (k >= 0) & (k < CHUNKS)
        kind = jnp.where(u < U1, 0, jnp.where(u < U2, 1, 2))
        return on(k0) | on(k1) | on(k2), kind, jnp.where(u < U1, k0, jnp.where(u < U2, k1, k2))

    def weights(u):
        on, kind, j = work(u)
        layer = jnp.where(kind == 1, 1, 0)
        slot = u % 2
        return on, (pltpu.make_async_copy(WGU.at[layer, :, pl.ds(pl.multiple_of(j * 2 * cw, 128), 2 * cw)], WC.at[slot], w_sem.at[slot, 0]),
                    pltpu.make_async_copy(WD.at[layer, pl.ds(pl.multiple_of(j * cw, 128), cw), :], WDC.at[slot], w_sem.at[slot, 1]))

    def forward(j, slot):
        gu = mm(A[...], WC[slot])
        g, up = gu[:, :cw], gu[:, cw:]
        ACT[...] = (g * jax.nn.sigmoid(g) * up).astype(BF16)
        @pl.when(j == 0)
        def _():
            DACC[...] = jnp.zeros_like(DACC)
        DACC[...] += mm(ACT[...], WDC[slot])

    def compute(j, slot):
        gu = mm(A[...], WC[slot])
        g, up = gu[:, :cw], gu[:, cw:]
        back = mm_nt(DY[...], WDC[slot]).astype(BF16).astype(F32)
        sg = jax.nn.sigmoid(g)
        s = g * sg
        ACT[...] = (s * up).astype(BF16)
        DGU[:, :cw] = (back * up * (sg + s * (1.0 - sg))).astype(BF16)
        DGU[:, cw:] = (back * s).astype(BF16)
        t = mm(AT[...], DGU[...]).astype(BF16)
        TS[0, j] = t[:, :cw]
        TS[1, j] = t[:, cw:]

    def compute_rest(kind, j, slot):
        @pl.when(kind == 1)
        def _():
            @pl.when(j == 0)
            def _():
                DACC[...] = jnp.zeros_like(DACC)
            DACC[...] += mm_nt(DGU[...], WC[slot])
        TD[jnp.where(kind == 1, 1, 0), pl.ds(pl.multiple_of(j * cw, 128), cw), :] = mm_tn(ACT[...], DY[...]).astype(BF16)

    def after_forward():
        def rows(i, _):
            rs = pl.ds(pl.multiple_of(i * 128, 128), 128)
            H[rs, :] = (H[rs, :].astype(F32) + DACC[rs, :].astype(BF16).astype(F32)).astype(BF16)
            return 0
        lax.fori_loop(0, tokens // 128, rows, 0)
        normalize(H, True)

    def between():
        xin = pltpu.make_async_copy(x, A, load_sem.at[0])
        xin.start()
        def rows(i, _):
            rs = pl.ds(pl.multiple_of(i * 128, 128), 128)
            wide = H[rs, :].astype(F32)
            scale = lax.rsqrt(jnp.mean(wide * wide, -1, keepdims=True) + 1e-6)
            da = DACC[rs, :].astype(BF16).astype(F32)
            dh = scale * da - wide * (scale * scale * scale * jnp.mean(wide * da, -1, keepdims=True))
            DY[rs, :] = (DY[rs, :].astype(F32) + dh.astype(BF16).astype(F32)).astype(BF16)
            return 0
        lax.fori_loop(0, tokens // 128, rows, 0)
        xin.wait()
        normalize(A, True)

    def item(i):
        return 1 - i // per, i % per

    def piece_of(layer, k, cc):
        return 2 * k + lax.rem(cc + layer, 2)

    def send_terms(i, start):
        layer, r = item(i)
        @pl.when(r < CHUNKS)
        def _():
            cp = remote(TS.at[1 - c, r], R.at[r], r_send, r_recv.at[i], dev(z, 1 - c))
            cp.start() if start else cp.wait_send()
        @pl.when(r >= CHUNKS)
        def _():
            k = r - CHUNKS
            p = piece_of(layer, k, 1 - c)
            @pl.when(p < PIECES)
            def _():
                if start:
                    for zz in range(nz):
                        rs = pl.ds(pl.multiple_of(zz * crd + p * prow, 16), prow)
                        remote(TD.at[layer, rs, :], RD.at[k, zz], r_send, r_recv.at[i], dev(z, 1 - c)).start()
                else:
                    wait(RD.at[k], r_send)

    def terms(i, zz, fn):
        layer, r = item(i)
        zz = lax.rem(zz + 2 * nz, nz)
        @pl.when(r < CHUNKS)
        def _():
            rs = pl.ds(pl.multiple_of(zz * 2 * rgu, 16), 2 * rgu)
            fn(TS.at[c, r, rs, :], R.at[r, rs, :], BG, r % 2, True)
        @pl.when(r >= CHUNKS)
        def _():
            k = r - CHUNKS
            p = piece_of(layer, k, c)
            @pl.when(p < PIECES)
            def _():
                fn(TD.at[layer, pl.ds(pl.multiple_of(zz * crd + p * prow, 16), prow), :], RD.at[k, zz], BD, k % 2, False)

    def ring_copy(i, way, s, buf):
        to = z + 1 if way == 0 else z - 1
        slot = i % SLOTS
        return remote(buf.at[way, s, slot], buf.at[way, s + 1, slot], ring_send.at[way, s, slot], ring_recv.at[way, s, slot], dev(to, c))

    def arrived(i, way, s, buf):
        slot = i % SLOTS
        wait(buf.at[way, s, slot], ring_recv.at[way, s - 1, slot])

    def stage(i, way, s):
        def fn_for(hops):
            def fn(own, other, buf, odd, is_gu):
                mine = (odd == way) if hops == half else (odd != way)
                @pl.when(mine)
                def _():
                    slot = i % SLOTS
                    t = own[...].astype(F32) + other[...].astype(F32)
                    if s > 0:
                        arrived(i, way, s, buf)
                        t = t + buf[way, s, slot].astype(F32)
                    buf[way, s, slot] = t.astype(BF16)
                    ring_copy(i, way, s, buf).start()
            return fn
        for hops in (half, half - 1):
            if s < hops:
                terms(i, z + (hops - s) if way == 0 else z - (hops - s), fn_for(hops))

    def stage_sent(i, way, s):
        def fn(own, other, buf, odd, is_gu):
            def go():
                ring_copy(i, way, s, buf).wait_send()
            if s < half - 1:
                go()
            else:
                pl.when(odd == way)(go)
        terms(i, z, fn)

    def last(i):
        layer, r = item(i)
        slot = i % SLOTS
        def fn(own, other, buf, odd, is_gu):
            def add(hops_up):
                t = own[...].astype(F32) + other[...].astype(F32)
                for way, hops in ((0, hops_up), (1, nz - 1 - hops_up)):
                    arrived(i, way, hops, buf)
                    t = t + buf[way, hops, slot].astype(F32)
                w = t.astype(BF16).astype(F32)
                sq = SQ[...]
                for a in range(w.shape[0] // 8):
                    for b in range(w.shape[1] // 128):
                        v = w[8 * a : 8 * a + 8, 128 * b : 128 * b + 128]
                        sq = sq + v * v
                SQ[...] = sq
                out, rows = (FG, rgu) if is_gu else (FD, prow // 2)
                out[slot, 0] = w[:rows].astype(BF16)
                out[slot, 1] = w[rows:].astype(BF16)
            @pl.when(odd == 0)
            def _():
                add(half)
            @pl.when(odd == 1)
            def _():
                add(half - 1)
            if is_gu:
                cs = pl.ds(pl.multiple_of(r * cw, 128), cw)
                pltpu.make_async_copy(FG.at[slot, c], ggu.at[layer, c, :, cs], fin_send.at[0, slot]).start()
                remote(FG.at[slot, 1 - c], ggu.at[layer, c, :, cs], fin_send.at[1, slot], fin_recv.at[layer, 0], dev(z, 1 - c)).start()
            else:
                p = piece_of(layer, r - CHUNKS, c)
                for b in range(2):
                    k = 2 * p + b
                    dst = gd.at[layer, pl.ds(pl.multiple_of(lax.rem(k, PIECES) * (prow // 2), 8), prow // 2), :]
                    @pl.when(k // PIECES == c)
                    def _():
                        pltpu.make_async_copy(FD.at[slot, b], dst, fin_send.at[b, slot]).start()
                    @pl.when(k // PIECES != c)
                    def _():
                        remote(FD.at[slot, b], dst, fin_send.at[b, slot], fin_recv.at[layer, 1], dev(z, 1 - c)).start()
        terms(i, z, fn)

    def last_sent(i):
        slot = i % SLOTS
        def fn(own, other, buf, odd, is_gu):
            for b in range(2):
                wait((FG if is_gu else FD).at[slot, b], fin_send.at[b, slot])
        terms(i, z, fn)

    def valid(i):
        return (i >= 0) & (i < total)

    def reduce_step(t):
        @pl.when(valid(t - 1))
        def _():
            send_terms(t - 1, False)
        for s in range(half):
            i = t - 2 - SK * s
            @pl.when(valid(i))
            def _():
                for way in (0, 1):
                    stage_sent(i, way, s)
        before = t - 2 - SK * half
        @pl.when(valid(before))
        def _():
            last_sent(before)
        final = t - 1 - SK * half
        @pl.when(valid(final))
        def _():
            last(final)
        for s in reversed(range(half)):
            i = t - 1 - SK * s
            @pl.when(valid(i))
            def _():
                if s == 0:
                    layer, r = item(i)
                    @pl.when(r < CHUNKS)
                    def _():
                        wait(R.at[r], r_recv.at[i])
                    @pl.when((r >= CHUNKS) & (piece_of(layer, r - CHUNKS, c) < PIECES))
                    def _():
                        wait(RD.at[r - CHUNKS], r_recv.at[i])
                for way in (0, 1):
                    stage(i, way, s)

    normalize(H, False)

    def step(u, _):
        t = u - U1
        @pl.when(u < gtotal + gdone)
        def _():
            gather_step(u)
        @pl.when(t >= 0)
        def _():
            reduce_step(t)

        on, kind, j = work(u)
        slot = u % 2
        following, loads = weights(u + 1)
        @pl.when(following)
        def _():
            for cp in loads:
                cp.start()
        @pl.when(u == U1 - 1)
        def _():
            after_forward()
        @pl.when(u == U2 - 1)
        def _():
            between()
        @pl.when(on)
        def _():
            for cp in weights(u)[1]:
                cp.wait()
        @pl.when(on & (kind == 0))
        def _():
            forward(j, slot)
        @pl.when(on & (kind > 0))
        def _():
            compute(j, slot)
        @pl.when(valid(t))
        def _():
            send_terms(t, True)
        @pl.when(on & (kind > 0))
        def _():
            compute_rest(kind, j, slot)
        return 0

    lax.fori_loop(0, U1 + total + SK * half + 2, step, 0)

    for i in range(1, n):
        remote(SQ, SQALL.at[me], sq_send, sq_recv, {"dp": lax.rem(me + i, n)}).start()
    for layer in range(2):
        wait(ggu.at[layer, 0], fin_recv.at[layer, 0])
        even = lax.rem(c + layer, 2) == 0
        @pl.when(even)
        def _():
            wait(gd.at[layer, pl.ds(0, PIECES // 2 * (prow // 2)), :], fin_recv.at[layer, 1])
        @pl.when(jnp.logical_not(even))
        def _():
            wait(gd.at[layer, pl.ds(0, (PIECES + 1) // 2 * (prow // 2)), :], fin_recv.at[layer, 1])
    wait(SQALL.at[pl.ds(0, n - 1)], sq_recv)
    acc = SQ[...]
    for i in range(1, n):
        acc = acc + SQALL[lax.rem(me + i, n)]
    sqo[...] = acc
    wait(SQALL.at[pl.ds(0, n - 1)], sq_send)


def train(mesh, x, dy, w_gate, w_up, w_down):
    n = mesh.shape["dp"]
    nz = n // 2
    half = nz // 2
    tokens, d = x.shape
    layers, rgu, ff = w_gate.shape
    rd = ff // n
    cw = ff // CHUNKS
    prow = 2 * rd // PIECES
    items = (PIECES + 1) // 2
    total = 2 * (CHUNKS + items)
    V, S = pltpu.VMEM, pltpu.SemaphoreType.DMA
    shape = jax.ShapeDtypeStruct
    return pl.pallas_call(
        functools.partial(train_kernel, nz, math.isqrt(mesh.shape["rep"])),
        out_shape=(
            shape((layers, 2, rgu, ff), BF16), shape((layers, rd, d), BF16), shape((8, 128), F32),
            shape((layers, d, 2 * ff), BF16), shape((layers, ff, d), BF16),
        ),
        in_specs=[ANY] * 5,
        out_specs=(ANY, ANY, pl.BlockSpec(memory_space=pltpu.VMEM), ANY, ANY),
        scratch_shapes=[
            V((tokens, d), BF16), V((tokens, d), BF16), V((tokens, d), BF16), V((d, tokens), BF16), V((tokens, d), F32),
            V((2, d, 2 * cw), BF16), V((2, cw, d), BF16), V((tokens, 2 * cw), BF16), V((tokens, cw), BF16),
            V((2, CHUNKS, d, cw), BF16), V((CHUNKS, d, cw), BF16), V((layers, ff, d), BF16), V((items, nz, prow, d), BF16),
            V((2, half + 1, SLOTS, 2 * rgu, cw), BF16), V((2, half + 1, SLOTS, prow, d), BF16),
            V((SLOTS, 2, rgu, cw), BF16), V((SLOTS, 2, prow // 2, d), BF16),
            V((8, 128), F32), V((n, 8, 128), F32), V((layers, rgu, 2 * ff), BF16), V((layers, rd, d), BF16),
            S((4,)), S((2, 2)), S((GSLOTS,)), S((2, half, RSLOTS)), S((GSLOTS,)), S((GSLOTS,)), S((GSLOTS,)),
            S, S((total,)), S((2, half, SLOTS)), S((2, half, SLOTS)), S((2, SLOTS)), S((layers, 2)), S, S,
        ],
        compiler_params=pltpu.CompilerParams(collective_id=0, has_side_effects=True, vmem_limit_bytes=63 * 2**20),
        name="train",
    )(x, dy, w_gate, w_up, w_down)


def adamw(w, m, v, g):
    m = 0.9 * m + 0.1 * g
    v = 0.95 * v + 0.05 * g * g
    step = m * lax.rsqrt(v + 1e-8) + 0.1 * w
    return (w - 0.02 * step).astype(BF16), m, v


def solution(mesh):
    n = mesh.shape["dp"]

    def step(x, dy, *arrays):
        weights, m, v = (arrays[i : i + 3] for i in (0, 3, 6))
        ggu, gd, squares = train(mesh, x[0], dy[0], *weights)[:3]
        gradients = [g.astype(F32) for g in (ggu[:, 0], ggu[:, 1], gd)]
        count = n * sum(g.size for g in gradients)
        factor = jnp.minimum(1.0, 0.5 * lax.rsqrt(jnp.sum(squares) / count + 1e-30))
        new = [adamw(w.astype(F32), m, v, g * factor) for w, m, v, g in zip(weights, m, v, gradients, strict=True)]
        return tuple(one[which] for which in range(3) for one in new)

    states, cut = P(("rep", "dp"), None, None), P(None, "dp", None)
    return jax.shard_map(
        step,
        mesh=mesh,
        in_specs=(states, states) + (cut,) * 9,
        out_specs=(P("rep", "dp", None),) * 9,
        check_vma=False,
    )
```

```python
import functools
import math

import jax
import jax.numpy as jnp
from jax import lax
from jax.experimental import pallas as pl
from jax.experimental.pallas import tpu as pltpu
from jax.sharding import PartitionSpec as P

MESH = pl.DeviceIdType.MESH
ANY = pl.BlockSpec(memory_space=pltpu.HBM)
F32, BF16 = jnp.float32, jnp.bfloat16
SK = 2
SLOTS = 8
GSLOTS = 16
RSLOTS = 8
GPAR = 2
GDONE = 2
GSK = 2
DCH = 3
CHUNKS = 9
SPREAD = 1
THREE = 3
PIECES = 9


def mm(a, b):
    return jnp.dot(a, b, preferred_element_type=F32)


def mm_nt(a, b):
    return lax.dot_general(a, b, (((1,), (1,)), ((), ())), preferred_element_type=F32)


def mm_tn(a, b):
    return lax.dot_general(a, b, (((0,), (0,)), ((), ())), preferred_element_type=F32)


def train_kernel(nz, ny, x, dy, wg, wu, wd, ggu, gd, sqo, WGU, WD, GUH, DGH, AH, ATH,
                 H, DY, A, AT, DACC, WC, WDC, GUS, DGU, ACT, TS, R, TD, RD, BG, BD, FG, FD, SQ, SQALL, sgu, sd,
                 load_sem, w_sem, gu_sem, dg_sem, own_sem, g_recv, g_sib, g_send, g_par,
                 r_send, r_recv, rd_send, rd_recv, ring_send, ring_recv, dring_send, dring_recv, fin_send, dfin_send, fin_recv, sq_send, sq_recv):
    me = lax.axis_index("dp")
    z, c = me // 2, me % 2
    n = 2 * nz
    half = nz // 2
    tokens, d = H.shape
    rgu = d // n
    cw = TS.shape[-1]
    ff = cw * CHUNKS
    rd = ff // n
    drow = rd // DCH
    crd = 2 * rd
    prow = crd // PIECES
    items = (PIECES + 1) // 2
    gper = DCH + CHUNKS
    gtotal = 2 * gper
    dhalf = (drow // 16 + 1) * 8
    gpar = GSK * half + GPAR
    gdone = gpar + GDONE
    UF = DCH + gdone + 1
    U1 = UF + CHUNKS
    UB = U1 + CHUNKS
    UC = UB + CHUNKS // THREE + 1
    G1, G0, D1, D0 = 1, UC - U1 + 1, CHUNKS + 1, UC - U1 + CHUNKS + 1

    def gathered(u):
        return jnp.where(u < UF, u, UF + lax.div(4 * (u - UF), 3))

    rep = lax.axis_index("rep")
    gx, gy = rep // ny, rep % ny
    diagonal = lax.rem(gx + gy, 2)
    beside_y = rep + 1 - 2 * lax.rem(gy, 2)
    beside_x = rep + ny * (1 - 2 * lax.rem(gx, 2))

    def dev(zz, cc):
        return {"dp": lax.rem(zz + nz, nz) * 2 + cc}

    up, down, sibling = dev(z + 1, c), dev(z - 1, c), dev(z, 1 - c)

    def remote(src, dst, s, r, to):
        return pltpu.make_async_remote_copy(src, dst, s, r, device_id=to, device_id_type=MESH)

    def wait(ref, sem):
        remote(ref, ref, sem, sem, sibling).wait_recv()

    first = [pltpu.make_async_copy(x, H, load_sem.at[0]), pltpu.make_async_copy(dy, DY, load_sem.at[1]), pltpu.make_async_copy(wd, sd, load_sem.at[2])]
    for cp in first:
        cp.start()
    for j in range(CHUNKS):
        for m, w in enumerate((wg, wu)):
            pltpu.make_async_copy(w.at[:, :, j * cw : (j + 1) * cw], sgu.at[:, j, m], load_sem.at[3]).start()

    barrier = pltpu.get_barrier_semaphore()
    for i in range(1, n):
        pl.semaphore_signal(barrier, inc=1, device_id={"dp": lax.rem(me + i, n)}, device_id_type=MESH)
    for to in (beside_x, beside_y):
        pl.semaphore_signal(barrier, inc=1, device_id={"rep": to, "dp": me}, device_id_type=MESH)
    pl.semaphore_wait(barrier, n + 1)
    for cp in first:
        cp.wait()
    pltpu.make_async_copy(WGU.at[:, :, :, :rgu, :], sgu, load_sem.at[3]).wait()

    SQ[...] = jnp.zeros_like(SQ)

    def normalize(src, transposed):
        def rows(i, _):
            rs = pl.ds(pl.multiple_of(i * 128, 128), 128)
            wide = src[rs, :].astype(F32)
            a = (wide * lax.rsqrt(jnp.mean(wide * wide, -1, keepdims=True) + 1e-6)).astype(BF16)
            A[rs, :] = a
            if transposed:
                AT[:, rs] = a.T
            return 0
        lax.fori_loop(0, tokens // 128, rows, 0)

    def chunk(q):
        layer = jnp.where(q >= gper, 1, 0)
        r = q - layer * gper
        return layer, r < DCH, jnp.where(r < DCH, r, r - DCH)

    def piece(q, blk, part, own, fn):
        layer, is_down, r = chunk(q)
        @pl.when(is_down)
        def _():
            def rows(first, size):
                here = pl.ds(pl.multiple_of(r * drow + first, 8), size)
                dst = WD.at[layer, pl.ds(pl.multiple_of(blk * rd + r * drow + first, 8), size), :]
                fn(sd.at[layer, here, :] if own else dst, dst)
            if part == 2:
                rows(0, drow)
            else:
                @pl.when(diagonal == part)
                def _():
                    rows(0, dhalf)
                @pl.when(diagonal != part)
                def _():
                    rows(dhalf, drow - dhalf)
        @pl.when(jnp.logical_not(is_down))
        def _():
            which = pl.ds(0, 2) if part == 2 else lax.rem(diagonal + part, 2)
            dst = WGU.at[layer, r, which, pl.ds(pl.multiple_of(blk * rgu, 8), rgu), :]
            fn(sgu.at[layer, r, which] if own else dst, dst)

    def block(zz):
        return jnp.where(zz >= nz, zz - nz, jnp.where(zz < 0, zz + nz, zz)) * 2 + c

    def to_sibling(q, src, dst):
        remote(src, dst, g_send.at[lax.rem(q, GSLOTS)], g_sib.at[lax.rem(q, GSLOTS)], sibling).start()

    def to_next(q, way, hop, src, dst):
        remote(src, dst, g_send.at[lax.rem(q, GSLOTS)], g_recv.at[way, hop - 1, lax.rem(q, RSLOTS)], (up, down)[way]).start()

    def to_beside(q, src, dst):
        to = jnp.where(lax.rem(q, 2) == 0, beside_y, beside_x)
        remote(src, dst, g_send.at[lax.rem(q, GSLOTS)], g_par.at[lax.rem(q, GSLOTS)], {"rep": to, "dp": me}).start()

    def gather_step(t):
        @pl.when(t < gtotal)
        def _():
            def own(src, dst):
                to_next(t, 0, 1, src, dst)
                to_next(t, 1, 1, src, dst)
            piece(t, me, 0, True, own)
            def whole(src, dst):
                to_sibling(t, src, dst)
                pltpu.make_async_copy(src, dst, own_sem.at[lax.rem(t, GSLOTS)]).start()
            piece(t, me, 2, True, whole)
        for h in range(1, half + 1):
            q = t - GSK * h
            for way in (0, 1):
                longer = lax.rem(q, 2) == way
                ok = (q >= 0) & (q < gtotal)
                if h == half:
                    ok = ok & longer
                @pl.when(ok)
                def _():
                    def go(src, dst):
                        remote(src, dst, g_send.at[0], g_recv.at[way, h - 1, lax.rem(q, RSLOTS)], sibling).wait_recv()
                        if h < half - 1:
                            to_next(q, way, h + 1, src, dst)
                        elif h == half - 1:
                            @pl.when(longer)
                            def _():
                                to_next(q, way, h + 1, src, dst)
                        to_beside(q, src, dst)
                    piece(q, block(z - h if way == 0 else z + h), 0, False, go)
        q = t - gpar
        @pl.when((q >= 0) & (q < gtotal))
        def _():
            layer, is_down, r = chunk(q)
            slot = lax.rem(q, GSLOTS)
            @pl.when(is_down)
            def _():
                for theirs in range(2):
                    @pl.when(diagonal != theirs)
                    def _():
                        wait(WD.at[layer, pl.ds(0, (nz - 1) * (drow - dhalf if theirs else dhalf)), :], g_par.at[slot])
            @pl.when(jnp.logical_not(is_down))
            def _():
                wait(WGU.at[layer, 0, 0, pl.ds(0, (nz - 1) * rgu), :], g_par.at[slot])
            for h in range(1, nz):
                piece(q, block(z + h), 2, False, lambda src, dst: to_sibling(q, src, dst))
        q = t - gdone
        @pl.when((q >= 0) & (q < gtotal))
        def _():
            layer, is_down, r = chunk(q)
            slot = lax.rem(q, GSLOTS)
            def waited(ref, sem):
                pltpu.make_async_copy(ref, ref, sem.at[slot]).wait()
            @pl.when(is_down)
            def _():
                rows = lambda k: WD.at[layer, pl.ds(0, k), :]
                waited(rows(drow), own_sem)
                waited(rows(nz * drow), g_sib)
                for mine in range(2):
                    @pl.when(diagonal == mine)
                    def _():
                        waited(rows(nz * drow + 2 * (nz - 1) * (drow - dhalf if mine else dhalf)), g_send)
            @pl.when(jnp.logical_not(is_down))
            def _():
                for k, sem in ((1, own_sem), (nz, g_sib), (2 * nz - 1, g_send)):
                    waited(WGU.at[layer, 0, :, pl.ds(0, k * rgu), :], sem)

    def work(u):
        ks = [u - first for first in (UF, U1, UB, UC)]
        on = functools.reduce(jnp.logical_or, [(k >= 0) & (k < (CHUNKS // THREE if first == UB else CHUNKS)) for k, first in zip(ks, (UF, U1, UB, UC))])
        pick = lambda a, b, c, d: jnp.where(u < U1, a, jnp.where(u < UB, b, jnp.where(u < UC, c, d)))
        return on, pick(0, 1, 2, 3), pick(*ks)

    def loads(u):
        on, kind, j = work(u)
        layer = jnp.where((kind == 0) | (kind == 3), 0, 1)
        slot = lax.rem(u, 2)
        return (
            (on & (kind < 2), pltpu.make_async_copy(WGU.at[layer, j, 0], WC.at[slot, :, pl.ds(0, cw)], w_sem.at[slot, 0])),
            (on & (kind < 2), pltpu.make_async_copy(WGU.at[layer, j, 1], WC.at[slot, :, pl.ds(cw, cw)], w_sem.at[slot, 1])),
            (on & (kind != 2), pltpu.make_async_copy(WD.at[layer, pl.ds(pl.multiple_of(j * cw, 128), cw), :], WDC.at[slot], w_sem.at[slot, 2])),
            (on & (kind == 3), pltpu.make_async_copy(GUH.at[j], GUS.at[slot], w_sem.at[slot, 4])),
        )

    def kept(j, slot, buf, hbm, sem):
        return pltpu.make_async_copy(buf.at[slot], hbm.at[j], sem.at[slot])

    def forward(j, slot):
        @pl.when(j >= 2)
        def _():
            kept(j, slot, GUS, GUH, gu_sem).wait()
        gu = mm(A[...], WC[slot])
        GUS[slot] = gu
        kept(j, slot, GUS, GUH, gu_sem).start()
        g, up = gu[:, :cw], gu[:, cw:]
        ACT[...] = (g * jax.nn.sigmoid(g) * up).astype(BF16)
        @pl.when(j == 0)
        def _():
            DACC[...] = jnp.zeros_like(DACC)
        DACC[...] += mm(ACT[...], WDC[slot])

    def down_gradient(layer, j):
        TD[layer, pl.ds(pl.multiple_of(j * cw, 128), cw), :] = mm_tn(ACT[...], DY[...]).astype(BF16)

    def backward(gu, j, slot):
        g, up = gu[:, :cw], gu[:, cw:]
        back = mm_nt(DY[...], WDC[slot]).astype(BF16).astype(F32)
        sg = jax.nn.sigmoid(g)
        s = g * sg
        ACT[...] = (s * up).astype(BF16)
        DGU[slot, :, :cw] = (back * up * (sg + s * (1.0 - sg))).astype(BF16)
        DGU[slot, :, cw:] = (back * s).astype(BF16)
        t = mm(AT[...], DGU[slot]).astype(BF16)
        TS[0, j] = t[:, :cw]
        TS[1, j] = t[:, cw:]

    def second_layer(j, slot):
        @pl.when(j >= 2)
        def _():
            kept(j, slot, DGU, DGH, dg_sem).wait()
        backward(mm(A[...], WC[slot]), j, slot)
        @pl.when(j < CHUNKS - 2)
        def _():
            kept(j, slot, DGU, DGH, dg_sem).start()

    def first_layer(j, slot):
        backward(GUS[slot], j, slot)

    def input_gradient(step):
        def again(k, slot):
            return (pltpu.make_async_copy(WGU.at[1, k, 0], WC.at[slot, :, pl.ds(0, cw)], w_sem.at[slot, 0]),
                    pltpu.make_async_copy(WGU.at[1, k, 1], WC.at[slot, :, pl.ds(cw, cw)], w_sem.at[slot, 1]),
                    pltpu.make_async_copy(DGH.at[k], DGU.at[slot], w_sem.at[slot, 3]))

        def one(i, _):
            m = THREE * step + i
            slot = lax.rem(m + U1 + CHUNKS, 2)
            @pl.when(m >= 2)
            def _():
                for copy in again(CHUNKS - 1 - m, slot):
                    copy.wait()
            @pl.when(m == 0)
            def _():
                DACC[...] = jnp.zeros_like(DACC)
            DACC[...] += mm_nt(DGU[slot], WC[slot])
            @pl.when(m + 2 < CHUNKS)
            def _():
                for copy in again(CHUNKS - 3 - m, slot):
                    copy.start()
            return 0
        lax.fori_loop(0, THREE, one, 0)

    def after_forward():
        def rows(i, _):
            rs = pl.ds(pl.multiple_of(i * 128, 128), 128)
            H[rs, :] = (H[rs, :].astype(F32) + DACC[rs, :].astype(BF16).astype(F32)).astype(BF16)
            return 0
        lax.fori_loop(0, tokens // 128, rows, 0)
        normalize(H, True)

    def between():
        def rows(i, _):
            rs = pl.ds(pl.multiple_of(i * 128, 128), 128)
            wide = H[rs, :].astype(F32)
            scale = lax.rsqrt(jnp.mean(wide * wide, -1, keepdims=True) + 1e-6)
            da = DACC[rs, :].astype(BF16).astype(F32)
            dh = scale * da - wide * (scale * scale * scale * jnp.mean(wide * da, -1, keepdims=True))
            DY[rs, :] = (DY[rs, :].astype(F32) + dh.astype(BF16).astype(F32)).astype(BF16)
            return 0
        lax.fori_loop(0, tokens // 128, rows, 0)

    class Item:
        pass

    def gu_item(t, s):
        e = Item()
        i = t - G1 - SK * s
        second = i < CHUNKS
        e.r = jnp.where(second, i, i - (G0 - G1))
        e.valid = (e.r >= 0) & (e.r < CHUNKS)
        e.layer = jnp.where(second, 1, 0)
        e.i, e.slot, e.odd, e.gu = i, lax.rem(i, SLOTS), lax.rem(e.r, 2), True
        e.buf, e.sent, e.come = BG, ring_send, ring_recv
        return e

    def d_item(t, s, layer):
        e = Item()
        if layer == 1:
            i = t - D1 - SK * s
            e.valid = (i >= 0) & (i < SPREAD * items) & (lax.rem(i, SPREAD) == 0)
            k = lax.div(i, SPREAD)
        else:
            k = t - D0 - s
            e.valid = (k >= 0) & (k < items)
        e.p = 2 * k + (1 - c if layer == 1 else c)
        e.valid = e.valid & (e.p < PIECES)
        e.k, e.layer, e.odd, e.gu = k, layer, lax.rem(k, 2), False
        e.slot = k
        e.buf, e.sent, e.come = BD, dring_send, dring_recv
        return e

    def terms(e, zz):
        if e.gu:
            rs = pl.ds(pl.multiple_of(zz * (2 * rgu), 16), 2 * rgu)
            return TS[c, e.r, rs, :].astype(F32) + R[e.r, rs, :].astype(F32)
        rs = pl.ds(pl.multiple_of(zz * crd + e.p * prow, 16), prow)
        return TD[e.layer, rs, :].astype(F32) + RD[e.slot, zz].astype(F32)

    def around(zz):
        return jnp.where(zz >= nz, zz - nz, jnp.where(zz < 0, zz + nz, zz))

    def ring_copy(e, way, s):
        return remote(e.buf.at[way, s, e.slot], e.buf.at[way, s + 1, e.slot], e.sent.at[way, s, e.slot], e.come.at[way, s, e.slot], (up, down)[way])

    def stage(e, s):
        def go(way):
            far = half - 1 - s + jnp.where(e.odd == way, 1, 0)
            t = terms(e, around(z + far if way == 0 else z - far))
            if s > 0:
                wait(e.buf.at[way, s, e.slot], e.come.at[way, s - 1, e.slot])
                t = t + e.buf[way, s, e.slot].astype(F32)
            e.buf[way, s, e.slot] = t.astype(BF16)
            ring_copy(e, way, s).start()
        if s < half - 1:
            @pl.when(e.valid)
            def _():
                go(0)
                go(1)
        else:
            for way in (0, 1):
                @pl.when(e.valid & (e.odd == way))
                def _():
                    go(way)

    def stage_sent(e, s):
        if s < half - 1:
            @pl.when(e.valid)
            def _():
                ring_copy(e, 0, s).wait_send()
                ring_copy(e, 1, s).wait_send()
        else:
            for way in (0, 1):
                @pl.when(e.valid & (e.odd == way))
                def _():
                    ring_copy(e, way, s).wait_send()

    def last(e):
        @pl.when(e.valid)
        def _():
            t = terms(e, z)
            for way in (0, 1):
                hops = half - 1 + jnp.where(e.odd == way, 1, 0)
                wait(e.buf.at[way, hops, e.slot], e.come.at[way, hops - 1, e.slot])
                t = t + e.buf[way, hops, e.slot].astype(F32)
            w = t.astype(BF16).astype(F32)
            sq = SQ[...]
            for a in range(w.shape[0] // 8):
                for b in range(w.shape[1] // 128):
                    v = w[8 * a : 8 * a + 8, 128 * b : 128 * b + 128]
                    sq = sq + v * v
            SQ[...] = sq
            out, rows = (FG, rgu) if e.gu else (FD, prow // 2)
            out[e.slot, 0] = w[:rows].astype(BF16)
            out[e.slot, 1] = w[rows:].astype(BF16)
            if e.gu:
                cs = pl.ds(pl.multiple_of(e.r * cw, 128), cw)
                pltpu.make_async_copy(FG.at[e.slot, c], ggu.at[e.layer, c, :, cs], fin_send.at[0, e.slot]).start()
                remote(FG.at[e.slot, 1 - c], ggu.at[e.layer, c, :, cs], fin_send.at[1, e.slot], fin_recv.at[e.layer, 0], sibling).start()
            else:
                for b in range(2):
                    k = 2 * e.p + b
                    theirs = k >= PIECES
                    row = jnp.where(theirs, k - PIECES, k) * (prow // 2)
                    dst = gd.at[e.layer, pl.ds(pl.multiple_of(row, 8), prow // 2), :]
                    owner = jnp.where(theirs, 1, 0)
                    @pl.when(owner == c)
                    def _():
                        pltpu.make_async_copy(FD.at[e.slot, b], dst, dfin_send.at[b, e.slot]).start()
                    @pl.when(owner != c)
                    def _():
                        remote(FD.at[e.slot, b], dst, dfin_send.at[b, e.slot], fin_recv.at[e.layer, 1], sibling).start()

    def last_sent(e):
        @pl.when(e.valid)
        def _():
            for b in range(2):
                if e.gu:
                    wait(FG.at[e.slot, b], fin_send.at[b, e.slot])
                else:
                    wait(FD.at[e.slot, b], dfin_send.at[b, e.slot])

    streams = (gu_item, lambda t, s: d_item(t, s, 1), lambda t, s: d_item(t, s, 0))

    def send_terms(t):
        e = gu_item(t + 1, 0)
        @pl.when(e.valid)
        def _():
            remote(TS.at[1 - c, e.r], R.at[e.r], r_send, r_recv.at[e.r], sibling).start()
        for layer in (1, 0):
            e = d_item(t + 1, 0, layer)
            p = 2 * e.k + (c if layer == 1 else 1 - c)
            there = d_valid(t + 1, layer) & (p < PIECES)
            @pl.when(there)
            def _():
                for zz in range(nz):
                    rs = pl.ds(pl.multiple_of(zz * crd + p * prow, 16), prow)
                    remote(TD.at[layer, rs, :], RD.at[e.slot, zz], rd_send, rd_recv.at[e.slot], sibling).start()

    def d_valid(t, layer):
        if layer == 1:
            i = t - D1
            return (i >= 0) & (i < SPREAD * items) & (lax.rem(i, SPREAD) == 0)
        return (t >= D0) & (t < D0 + items)

    def terms_sent(t):
        e = gu_item(t + 1, 0)
        @pl.when(e.valid)
        def _():
            wait(R.at[e.r], r_send)
        for layer in (1, 0):
            e = d_item(t + 1, 0, layer)
            p = 2 * e.k + (c if layer == 1 else 1 - c)
            @pl.when(d_valid(t + 1, layer) & (p < PIECES))
            def _():
                wait(RD.at[e.slot], rd_send)

    def reduce_step(t):
        terms_sent(t - 1)
        for which in streams:
            for s in range(half):
                stage_sent(which(t - 1, s), s)
            last_sent(which(t - 1, half))
        for some in (streams[:2], streams[2:]):
            for which in some:
                last(which(t, half))
            for s in reversed(range(half)):
                for which in some:
                    e = which(t, s)
                    if s == 0:
                        @pl.when(e.valid)
                        def _():
                            if e.gu:
                                wait(R.at[e.r], r_recv.at[e.r])
                            else:
                                wait(RD.at[e.slot], rd_recv.at[e.slot])
                    stage(e, s)

    normalize(H, True)
    keep = (pltpu.make_async_copy(A, AH, load_sem.at[0]), pltpu.make_async_copy(AT, ATH, load_sem.at[1]))
    back = (pltpu.make_async_copy(AH, A, load_sem.at[0]), pltpu.make_async_copy(ATH, AT, load_sem.at[1]))
    for copy in keep:
        copy.start()

    def step(u, _):
        t = u - U1
        @pl.when(gathered(u) < gtotal + gdone)
        def _():
            def one(tg, _):
                gather_step(tg)
                return 0
            lax.fori_loop(gathered(u), gathered(u + 1), one, 0)
        @pl.when(t >= 0)
        def _():
            reduce_step(t)

        on, kind, j = work(u)
        slot = lax.rem(u, 2)
        @pl.when((u == UF + CHUNKS) | (u == UF + CHUNKS + 1))
        def _():
            kept(0, slot, GUS, GUH, gu_sem).wait()
        for there, copy in loads(u + 1):
            @pl.when(there)
            def _():
                copy.start()
        @pl.when(u == U1)
        def _():
            for copy in keep:
                copy.wait()
            after_forward()
        @pl.when(u == UB)
        def _():
            for copy in back:
                copy.start()
        @pl.when(u == UC - 1)
        def _():
            between()
            for copy in back:
                copy.wait()
        for there, copy in loads(u):
            @pl.when(there)
            def _():
                copy.wait()
        @pl.when(on & (kind == 0))
        def _():
            forward(j, slot)
        @pl.when(on & (kind == 1))
        def _():
            second_layer(j, slot)
        @pl.when(on & (kind == 3))
        def _():
            first_layer(j, slot)
        @pl.when(t >= 0)
        def _():
            send_terms(t)
        @pl.when(on & (kind == 1))
        def _():
            down_gradient(1, j)
        @pl.when(on & (kind == 2))
        def _():
            input_gradient(j)
        @pl.when(on & (kind == 3))
        def _():
            down_gradient(0, j)
        return 0

    lax.fori_loop(0, U1 + D0 + items + half + 1, step, 0)

    for i in range(1, n):
        remote(SQ, SQALL.at[me], sq_send, sq_recv, {"dp": lax.rem(me + i, n)}).start()
    for layer in range(2):
        wait(ggu.at[layer, 0], fin_recv.at[layer, 0])
        even = lax.rem(c + layer, 2) == 0
        @pl.when(even)
        def _():
            wait(gd.at[layer, pl.ds(0, PIECES // 2 * (prow // 2)), :], fin_recv.at[layer, 1])
        @pl.when(jnp.logical_not(even))
        def _():
            wait(gd.at[layer, pl.ds(0, (PIECES + 1) // 2 * (prow // 2)), :], fin_recv.at[layer, 1])
    wait(SQALL.at[pl.ds(0, n - 1)], sq_recv)
    acc = SQ[...]
    for i in range(1, n):
        acc = acc + SQALL[lax.rem(me + i, n)]
    sqo[...] = jnp.full((8, 128), jnp.sum(acc), F32)
    wait(SQALL.at[pl.ds(0, n - 1)], sq_send)


def train(mesh, x, dy, w_gate, w_up, w_down):
    n = mesh.shape["dp"]
    nz = n // 2
    half = nz // 2
    tokens, d = x.shape
    layers, rgu, ff = w_gate.shape
    rd = ff // n
    cw = ff // CHUNKS
    prow = 2 * rd // PIECES
    items = (PIECES + 1) // 2
    V, S = pltpu.VMEM, pltpu.SemaphoreType.DMA
    shape = jax.ShapeDtypeStruct
    return pl.pallas_call(
        functools.partial(train_kernel, nz, math.isqrt(mesh.shape["rep"])),
        out_shape=(
            shape((layers, 2, rgu, ff), BF16), shape((layers, rd, d), BF16), shape((8, 128), F32),
            shape((layers, CHUNKS, 2, d, cw), BF16), shape((layers, ff, d), BF16),
            shape((CHUNKS, tokens, 2 * cw), F32), shape((CHUNKS, tokens, 2 * cw), BF16),
            shape((tokens, d), BF16), shape((d, tokens), BF16),
        ),
        in_specs=[ANY] * 5,
        out_specs=(ANY, ANY, pl.BlockSpec(memory_space=pltpu.VMEM), ANY, ANY, ANY, ANY, ANY, ANY),
        scratch_shapes=[
            V((tokens, d), BF16), V((tokens, d), BF16), V((tokens, d), BF16), V((d, tokens), BF16), V((tokens, d), F32),
            V((2, d, 2 * cw), BF16), V((2, cw, d), BF16), V((2, tokens, 2 * cw), F32), V((2, tokens, 2 * cw), BF16), V((tokens, cw), BF16),
            V((2, CHUNKS, d, cw), BF16), V((CHUNKS, d, cw), BF16), V((layers, ff, d), BF16), V((items, nz, prow, d), BF16),
            V((2, half + 1, SLOTS, 2 * rgu, cw), BF16), V((2, half + 1, items, prow, d), BF16),
            V((SLOTS, 2, rgu, cw), BF16), V((items, 2, prow // 2, d), BF16),
            V((8, 128), F32), V((n, 8, 128), F32), V((layers, CHUNKS, 2, rgu, cw), BF16), V((layers, rd, d), BF16),
            S((4,)), S((2, 5)), S((2,)), S((2,)), S((GSLOTS,)), S((2, half, RSLOTS)), S((GSLOTS,)), S((GSLOTS,)), S((GSLOTS,)),
            S, S((CHUNKS,)), S, S((items,)), S((2, half, SLOTS)), S((2, half, SLOTS)), S((2, half, items)), S((2, half, items)),
            S((2, SLOTS)), S((2, items)), S((layers, 2)), S, S,
        ],
        compiler_params=pltpu.CompilerParams(collective_id=0, has_side_effects=True, vmem_limit_bytes=63 * 2**20),
        name="train",
    )(x, dy, w_gate, w_up, w_down)


def adamw(w, m, v, g):
    m = 0.9 * m + 0.1 * g
    v = 0.95 * v + 0.05 * g * g
    step = m * lax.rsqrt(v + 1e-8) + 0.1 * w
    return (w - 0.02 * step).astype(BF16), m, v


def solution(mesh):
    n = mesh.shape["dp"]

    def step(x, dy, *arrays):
        weights, m, v = (arrays[i : i + 3] for i in (0, 3, 6))
        ggu, gd, squares = train(mesh, x[0], dy[0], *weights)[:3]
        gradients = [g.astype(F32) for g in (ggu[:, 0], ggu[:, 1], gd)]
        count = n * sum(g.size for g in gradients)
        factor = jnp.minimum(1.0, 0.5 * lax.rsqrt(squares[0, 0] / count + 1e-30))
        new = [adamw(w.astype(F32), m, v, g * factor) for w, m, v, g in zip(weights, m, v, gradients, strict=True)]
        return tuple(one[which] for which in range(3) for one in new)

    states, cut = P(("rep", "dp"), None, None), P(None, "dp", None)
    return jax.shard_map(
        step,
        mesh=mesh,
        in_specs=(states, states) + (cut,) * 9,
        out_specs=(P("rep", "dp", None),) * 9,
        check_vma=False,
    )
```

```python
import functools
import math

import jax
import jax.numpy as jnp
from jax import lax
from jax.experimental import pallas as pl
from jax.experimental.pallas import tpu as pltpu
from jax.sharding import PartitionSpec as P

MESH = pl.DeviceIdType.MESH
ANY = pl.BlockSpec(memory_space=pltpu.HBM)
F32, BF16 = jnp.float32, jnp.bfloat16
LAG = 3
SK = 2
DSLOTS = 8
SLOTS = 8
GSLOTS = 16
RSLOTS = 8
GPAR = 2
GDONE = 2
GSK = 2
DCH = 3
CHUNKS = 9
THREE = 3
PARTS = 2
PIECES = 9


def mm(a, b):
    return jnp.dot(a, b, preferred_element_type=F32)


def mm_nt(a, b):
    return lax.dot_general(a, b, (((1,), (1,)), ((), ())), preferred_element_type=F32)


def mm_tn(a, b):
    return lax.dot_general(a, b, (((0,), (0,)), ((), ())), preferred_element_type=F32)


def train_kernel(nz, ny, x, dy, wg, wu, wd, ggu, gd, sqo, WGU, WD, GUH, DGH, ACTH, AH, ATH,
                 H, DY, A, AT, DACC, WC, WDC, GUS, DGU, ACT, TS, R, TD, RD, BG, BD, FG, FD, SQ, SQALL, sgu, sd,
                 load_sem, w_sem, gu_sem, dg_sem, act_sem, own_sem, g_recv, g_sib, g_send, g_par,
                 r_send, r_recv, rd_send, rd_recv, ring_send, ring_recv, dring_send, dring_recv, fin_send, dfin_send, fin_recv, sq_send, sq_recv):
    me = lax.axis_index("dp")
    z, c = me // 2, me % 2
    n = 2 * nz
    half = nz // 2
    tokens, d = H.shape
    rgu = d // n
    cw = TS.shape[-1]
    ff = cw * CHUNKS
    rd = ff // n
    drow = rd // DCH
    crd = 2 * rd
    prow = crd // PIECES
    items = (PIECES + 1) // 2
    gper = DCH + CHUNKS
    gtotal = 2 * gper
    dhalf = (drow // 16 + 1) * 8
    gpar = GSK * half + GPAR
    gdone = gpar + GDONE
    UF = gdone + 1
    UE = UF + CHUNKS + DCH - 1
    U1 = UE + CHUNKS // THREE
    UB = U1 + CHUNKS
    UD = UB + CHUNKS // THREE
    UC = UD + 2
    G1, G0, D1 = 1, UC - U1 + 1, UC - U1 + 1 - items

    early = gper + DCH
    gsteps = early + 2 * (gtotal - 1 - early) + gdone + 1

    def gathered(u):
        return jnp.where(u < UE, u, UE + jnp.where(u < U1, lax.div(4 * (u - UE), 3), 4 * (U1 - UE) // 3 + 2 * (u - U1)))

    def started(t):
        late = t - early
        return (t >= 0) & ((late <= 0) | ((lax.rem(late, 2) == 0) & (t < gsteps - gdone))), jnp.where(late > 0, early + lax.div(late, 2), t)

    rep = lax.axis_index("rep")
    gx, gy = rep // ny, rep % ny
    diagonal = lax.rem(gx + gy, 2)
    beside_y = rep + 1 - 2 * lax.rem(gy, 2)
    beside_x = rep + ny * (1 - 2 * lax.rem(gx, 2))

    def dev(zz, cc):
        return {"dp": lax.rem(zz + nz, nz) * 2 + cc}

    up, down, sibling = dev(z + 1, c), dev(z - 1, c), dev(z, 1 - c)

    def remote(src, dst, s, r, to):
        return pltpu.make_async_remote_copy(src, dst, s, r, device_id=to, device_id_type=MESH)

    def wait(ref, sem):
        remote(ref, ref, sem, sem, sibling).wait_recv()

    first = [pltpu.make_async_copy(x, H, load_sem.at[0]), pltpu.make_async_copy(dy, DY, load_sem.at[1]), pltpu.make_async_copy(wd, sd, load_sem.at[2])]
    for cp in first:
        cp.start()
    for j in range(CHUNKS):
        for m, w in enumerate((wg, wu)):
            pltpu.make_async_copy(w.at[:, :, j * cw : (j + 1) * cw], sgu.at[:, j, m], load_sem.at[3]).start()

    barrier = pltpu.get_barrier_semaphore()
    for i in range(1, n):
        pl.semaphore_signal(barrier, inc=1, device_id={"dp": lax.rem(me + i, n)}, device_id_type=MESH)
    for to in (beside_x, beside_y):
        pl.semaphore_signal(barrier, inc=1, device_id={"rep": to, "dp": me}, device_id_type=MESH)
    pl.semaphore_wait(barrier, n + 1)
    for cp in first:
        cp.wait()
    pltpu.make_async_copy(WGU.at[:, :, :, :rgu, :], sgu, load_sem.at[3]).wait()

    SQ[...] = jnp.zeros_like(SQ)

    def normalize(src, transposed):
        def rows(i, _):
            rs = pl.ds(pl.multiple_of(i * 128, 128), 128)
            wide = src[rs, :].astype(F32)
            a = (wide * lax.rsqrt(jnp.mean(wide * wide, -1, keepdims=True) + 1e-6)).astype(BF16)
            A[rs, :] = a
            if transposed:
                AT[:, rs] = a.T
            return 0
        lax.fori_loop(0, tokens // 128, rows, 0)

    def chunk(q):
        second = q >= gper
        r = jnp.where(second, q - gper, q)
        down = jnp.where(second, r, r - CHUNKS)
        is_down = (down >= 0) & (down < DCH)
        return jnp.where(second, 1, 0), is_down, jnp.where(is_down, down, jnp.where(second, r - DCH, r))

    def piece(q, blk, part, own, fn):
        layer, is_down, r = chunk(q)
        @pl.when(is_down)
        def _():
            def rows(first, size):
                here = pl.ds(pl.multiple_of(r * drow + first, 8), size)
                dst = WD.at[layer, pl.ds(pl.multiple_of(blk * rd + r * drow + first, 8), size), :]
                fn(sd.at[layer, here, :] if own else dst, dst)
            if part == 2:
                rows(0, drow)
            else:
                @pl.when(diagonal == part)
                def _():
                    rows(0, dhalf)
                @pl.when(diagonal != part)
                def _():
                    rows(dhalf, drow - dhalf)
        @pl.when(jnp.logical_not(is_down))
        def _():
            which = pl.ds(0, 2) if part == 2 else lax.rem(diagonal + part, 2)
            dst = WGU.at[layer, r, which, pl.ds(pl.multiple_of(blk * rgu, 8), rgu), :]
            fn(sgu.at[layer, r, which] if own else dst, dst)

    def block(zz):
        return jnp.where(zz >= nz, zz - nz, jnp.where(zz < 0, zz + nz, zz)) * 2 + c

    def to_sibling(q, src, dst):
        remote(src, dst, g_send.at[lax.rem(q, GSLOTS)], g_sib.at[lax.rem(q, GSLOTS)], sibling).start()

    def to_next(q, way, hop, src, dst):
        remote(src, dst, g_send.at[lax.rem(q, GSLOTS)], g_recv.at[way, hop - 1, lax.rem(q, RSLOTS)], (up, down)[way]).start()

    def to_beside(q, src, dst):
        to = jnp.where(lax.rem(q, 2) == 0, beside_y, beside_x)
        remote(src, dst, g_send.at[lax.rem(q, GSLOTS)], g_par.at[lax.rem(q, GSLOTS)], {"rep": to, "dp": me}).start()

    def gather_step(t):
        def start(q):
            def own(src, dst):
                to_next(q, 0, 1, src, dst)
                to_next(q, 1, 1, src, dst)
            piece(q, me, 0, True, own)
            def whole(src, dst):
                to_sibling(q, src, dst)
                pltpu.make_async_copy(src, dst, own_sem.at[lax.rem(q, GSLOTS)]).start()
            piece(q, me, 2, True, whole)
        there, first = started(t)
        pl.when(there)(lambda: start(first))
        for h in range(1, half + 1):
            there, q = started(t - GSK * h)
            for way in (0, 1):
                longer = lax.rem(q, 2) == way
                ok = there
                if h == half:
                    ok = ok & longer
                @pl.when(ok)
                def _():
                    def go(src, dst):
                        remote(src, dst, g_send.at[0], g_recv.at[way, h - 1, lax.rem(q, RSLOTS)], sibling).wait_recv()
                        if h < half - 1:
                            to_next(q, way, h + 1, src, dst)
                        elif h == half - 1:
                            @pl.when(longer)
                            def _():
                                to_next(q, way, h + 1, src, dst)
                        to_beside(q, src, dst)
                    piece(q, block(z - h if way == 0 else z + h), 0, False, go)
        there, q = started(t - gpar)
        @pl.when(there)
        def _():
            layer, is_down, r = chunk(q)
            slot = lax.rem(q, GSLOTS)
            @pl.when(is_down)
            def _():
                for theirs in range(2):
                    @pl.when(diagonal != theirs)
                    def _():
                        wait(WD.at[layer, pl.ds(0, (nz - 1) * (drow - dhalf if theirs else dhalf)), :], g_par.at[slot])
            @pl.when(jnp.logical_not(is_down))
            def _():
                wait(WGU.at[layer, 0, 0, pl.ds(0, (nz - 1) * rgu), :], g_par.at[slot])
            for h in range(1, nz):
                piece(q, block(z + h), 2, False, lambda src, dst: to_sibling(q, src, dst))
        there, q = started(t - gdone)
        @pl.when(there)
        def _():
            layer, is_down, r = chunk(q)
            slot = lax.rem(q, GSLOTS)
            def waited(ref, sem):
                pltpu.make_async_copy(ref, ref, sem.at[slot]).wait()
            @pl.when(is_down)
            def _():
                rows = lambda k: WD.at[layer, pl.ds(0, k), :]
                waited(rows(drow), own_sem)
                waited(rows(nz * drow), g_sib)
                for mine in range(2):
                    @pl.when(diagonal == mine)
                    def _():
                        waited(rows(nz * drow + 2 * (nz - 1) * (drow - dhalf if mine else dhalf)), g_send)
            @pl.when(jnp.logical_not(is_down))
            def _():
                for k, sem in ((1, own_sem), (nz, g_sib), (2 * nz - 1, g_send)):
                    waited(WGU.at[layer, 0, :, pl.ds(0, k * rgu), :], sem)

    def work(u):
        ks = [u - first for first in (UF, U1, UC)]
        on = functools.reduce(jnp.logical_or, [(k >= 0) & (k < CHUNKS) for k in ks])
        pick = lambda a, b, c: jnp.where(u < UE, a, jnp.where(u < UC, b, c))
        return on, pick(0, 1, 3), pick(*ks)

    def loads(u):
        on, kind, j = work(u)
        layer = jnp.where((kind == 0) | (kind == 3), 0, 1)
        slot = lax.rem(u, 2)
        return (
            (on & (kind < 2), pltpu.make_async_copy(WGU.at[layer, j, 0], WC.at[slot, :, pl.ds(0, cw)], w_sem.at[slot, 0])),
            (on & (kind < 2), pltpu.make_async_copy(WGU.at[layer, j, 1], WC.at[slot, :, pl.ds(cw, cw)], w_sem.at[slot, 1])),
            (on & (kind > 0), pltpu.make_async_copy(WD.at[layer, pl.ds(pl.multiple_of(j * cw, 128), cw), :], WDC.at[slot], w_sem.at[slot, 2])),
            (on & (kind == 3), pltpu.make_async_copy(GUH.at[j], GUS.at[slot], w_sem.at[slot, 4])),
        )

    def kept(j, slot, buf, hbm, sem):
        return pltpu.make_async_copy(buf.at[slot], hbm.at[j], sem.at[slot])

    def forward(j, slot):
        @pl.when(j >= 2)
        def _():
            kept(j, slot, GUS, GUH, gu_sem).wait()
            kept(j, slot, ACT, ACTH, act_sem).wait()
        gu = mm(A[...], WC[slot])
        GUS[slot] = gu
        kept(j, slot, GUS, GUH, gu_sem).start()
        g, up = gu[:, :cw], gu[:, cw:]
        ACT[slot] = (g * jax.nn.sigmoid(g) * up).astype(BF16)
        kept(j, slot, ACT, ACTH, act_sem).start()

    def nth(m):
        return jnp.where(m < 2, CHUNKS - 2 + m, CHUNKS - 1 - m)

    def down_rows(m, slot):
        return pltpu.make_async_copy(WD.at[0, pl.ds(pl.multiple_of(nth(m) * cw, 128), cw), :], WDC.at[slot], w_sem.at[slot, 2])

    def forward_down(step):
        def one(i, _):
            m = THREE * step + i
            slot = lax.rem(m + UF + CHUNKS, 2)
            act = lambda k: pltpu.make_async_copy(ACTH.at[k], ACT.at[slot], act_sem.at[slot])
            down_rows(m, slot).wait()
            @pl.when(m >= 2)
            def _():
                act(0).wait()
            @pl.when(m == 0)
            def _():
                DACC[...] = jnp.zeros_like(DACC)
            DACC[...] += mm(ACT[slot], WDC[slot])
            @pl.when(m + 2 < CHUNKS)
            def _():
                down_rows(m + 2, slot).start()
                act(nth(m + 2)).start()
            return 0
        lax.fori_loop(0, THREE, one, 0)

    def down_gradient(layer, j, slot):
        TD[layer, pl.ds(pl.multiple_of(j * cw, 128), cw), :] = mm_tn(ACT[slot], DY[...]).astype(BF16)

    def kept_act(k):
        slot = lax.rem(k, 2)
        return pltpu.make_async_copy(ACTH.at[k], ACT.at[slot], act_sem.at[slot])

    def down_gradients(first, last):
        def one(k, _):
            kept_act(k).wait()
            down_gradient(0, k, lax.rem(k, 2))
            @pl.when(k + 2 < CHUNKS)
            def _():
                kept_act(k + 2).start()
            return 0
        lax.fori_loop(first, last, one, 0)

    def backward(products, j, slot, with_act):
        for first in range(0, tokens, tokens // PARTS):
            rs = pl.ds(first, tokens // PARTS)
            gu = products(rs)
            g, up = gu[:, :cw], gu[:, cw:]
            back = mm_nt(DY[rs, :], WDC[slot]).astype(BF16).astype(F32)
            sg = jax.nn.sigmoid(g)
            s = g * sg
            if with_act:
                ACT[slot, rs, :] = (s * up).astype(BF16)
            DGU[slot, rs, :cw] = (back * up * (sg + s * (1.0 - sg))).astype(BF16)
            DGU[slot, rs, cw:] = (back * s).astype(BF16)
        t = mm(AT[...], DGU[slot]).astype(BF16)
        TS[0, j] = t[:, :cw]
        TS[1, j] = t[:, cw:]

    def second_layer(j, slot):
        @pl.when(j >= 2)
        def _():
            kept(j, slot, DGU, DGH, dg_sem).wait()
        backward(lambda rs: mm(A[rs, :], WC[slot]), j, slot, True)
        @pl.when(j < CHUNKS - 2)
        def _():
            kept(j, slot, DGU, DGH, dg_sem).start()

    def first_layer(j, slot):
        backward(lambda rs: GUS[slot, rs, :], j, slot, False)

    def input_gradient(step):
        def again(k, slot):
            return (pltpu.make_async_copy(WGU.at[1, k, 0], WC.at[slot, :, pl.ds(0, cw)], w_sem.at[slot, 0]),
                    pltpu.make_async_copy(WGU.at[1, k, 1], WC.at[slot, :, pl.ds(cw, cw)], w_sem.at[slot, 1]),
                    pltpu.make_async_copy(DGH.at[k], DGU.at[slot], w_sem.at[slot, 3]))

        def one(i, _):
            m = THREE * step + i
            slot = lax.rem(m + U1 + CHUNKS, 2)
            @pl.when(m >= 2)
            def _():
                for copy in again(CHUNKS - 1 - m, slot):
                    copy.wait()
            @pl.when(m == 0)
            def _():
                DACC[...] = jnp.zeros_like(DACC)
            DACC[...] += mm_nt(DGU[slot], WC[slot])
            @pl.when(m + 2 < CHUNKS)
            def _():
                for copy in again(CHUNKS - 3 - m, slot):
                    copy.start()
            return 0
        lax.fori_loop(0, THREE, one, 0)

    def after_forward():
        def rows(i, _):
            rs = pl.ds(pl.multiple_of(i * 128, 128), 128)
            H[rs, :] = (H[rs, :].astype(F32) + DACC[rs, :].astype(BF16).astype(F32)).astype(BF16)
            return 0
        lax.fori_loop(0, tokens // 128, rows, 0)
        normalize(H, True)

    def between():
        def rows(i, _):
            rs = pl.ds(pl.multiple_of(i * 128, 128), 128)
            wide = H[rs, :].astype(F32)
            scale = lax.rsqrt(jnp.mean(wide * wide, -1, keepdims=True) + 1e-6)
            da = DACC[rs, :].astype(BF16).astype(F32)
            dh = scale * da - wide * (scale * scale * scale * jnp.mean(wide * da, -1, keepdims=True))
            DY[rs, :] = (DY[rs, :].astype(F32) + dh.astype(BF16).astype(F32)).astype(BF16)
            return 0
        lax.fori_loop(0, tokens // 128, rows, 0)

    class Item:
        pass

    def gu_item(t, s):
        e = Item()
        i = t - G1 - SK * s
        second = i < CHUNKS
        e.r = jnp.where(second, i, i - (G0 - G1))
        e.valid = (e.r >= 0) & (e.r < CHUNKS)
        e.layer = jnp.where(second, 1, 0)
        e.i, e.slot, e.odd, e.gu = i, lax.rem(i, SLOTS), lax.rem(e.r, 2), True
        e.buf, e.sent, e.come = BG, ring_send, ring_recv
        return e

    def d_item(t, s):
        e = Item()
        i = t - D1 - SK * s
        e.valid = (i >= 0) & (i < 2 * items)
        e.layer = jnp.where(i < items, 1, 0)
        k = i - (1 - e.layer) * items
        mine = jnp.where(e.layer == c, 0, 1)
        e.p, e.theirs = 2 * k + mine, 2 * k + 1 - mine
        e.sends, e.valid = e.valid & (e.theirs < PIECES), e.valid & (e.p < PIECES)
        e.i, e.slot, e.odd, e.gu = i, lax.rem(i, DSLOTS), lax.rem(k, 2), False
        e.buf, e.sent, e.come = BD, dring_send, dring_recv
        return e

    def terms(e, zz):
        if e.gu:
            rs = pl.ds(pl.multiple_of(zz * (2 * rgu), 16), 2 * rgu)
            return TS[c, e.r, rs, :].astype(F32) + R[e.r, rs, :].astype(F32)
        rs = pl.ds(pl.multiple_of(zz * crd + e.p * prow, 16), prow)
        return TD[e.layer, rs, :].astype(F32) + RD[e.i, zz].astype(F32)

    def around(zz):
        return jnp.where(zz >= nz, zz - nz, jnp.where(zz < 0, zz + nz, zz))

    def ring_copy(e, way, s):
        return remote(e.buf.at[way, s, e.slot], e.buf.at[way, s + 1, e.slot], e.sent.at[way, s, e.slot], e.come.at[way, s, e.slot], (up, down)[way])

    def stage(e, s):
        def go(way):
            far = half - 1 - s + jnp.where(e.odd == way, 1, 0)
            t = terms(e, around(z + far if way == 0 else z - far))
            if s > 0:
                wait(e.buf.at[way, s, e.slot], e.come.at[way, s - 1, e.slot])
                t = t + e.buf[way, s, e.slot].astype(F32)
            e.buf[way, s, e.slot] = t.astype(BF16)
            ring_copy(e, way, s).start()
        if s < half - 1:
            @pl.when(e.valid)
            def _():
                go(0)
                go(1)
        else:
            for way in (0, 1):
                @pl.when(e.valid & (e.odd == way))
                def _():
                    go(way)

    def stage_sent(e, s):
        if s < half - 1:
            @pl.when(e.valid)
            def _():
                ring_copy(e, 0, s).wait_send()
                ring_copy(e, 1, s).wait_send()
        else:
            for way in (0, 1):
                @pl.when(e.valid & (e.odd == way))
                def _():
                    ring_copy(e, way, s).wait_send()

    def last(e):
        @pl.when(e.valid)
        def _():
            t = terms(e, z)
            for way in (0, 1):
                hops = half - 1 + jnp.where(e.odd == way, 1, 0)
                wait(e.buf.at[way, hops, e.slot], e.come.at[way, hops - 1, e.slot])
                t = t + e.buf[way, hops, e.slot].astype(F32)
            w = t.astype(BF16).astype(F32)
            sq = SQ[...]
            for a in range(w.shape[0] // 8):
                for b in range(w.shape[1] // 128):
                    v = w[8 * a : 8 * a + 8, 128 * b : 128 * b + 128]
                    sq = sq + v * v
            SQ[...] = sq
            out, rows = (FG, rgu) if e.gu else (FD, prow // 2)
            out[e.slot, 0] = w[:rows].astype(BF16)
            out[e.slot, 1] = w[rows:].astype(BF16)
            if e.gu:
                cs = pl.ds(pl.multiple_of(e.r * cw, 128), cw)
                pltpu.make_async_copy(FG.at[e.slot, c], ggu.at[e.layer, c, :, cs], fin_send.at[0, e.slot]).start()
                remote(FG.at[e.slot, 1 - c], ggu.at[e.layer, c, :, cs], fin_send.at[1, e.slot], fin_recv.at[e.layer, 0], sibling).start()
            else:
                for b in range(2):
                    k = 2 * e.p + b
                    theirs = k >= PIECES
                    row = jnp.where(theirs, k - PIECES, k) * (prow // 2)
                    dst = gd.at[e.layer, pl.ds(pl.multiple_of(row, 8), prow // 2), :]
                    owner = jnp.where(theirs, 1, 0)
                    @pl.when(owner == c)
                    def _():
                        pltpu.make_async_copy(FD.at[e.slot, b], dst, dfin_send.at[b, e.slot]).start()
                    @pl.when(owner != c)
                    def _():
                        remote(FD.at[e.slot, b], dst, dfin_send.at[b, e.slot], fin_recv.at[e.layer, 1], sibling).start()

    def last_sent(e):
        @pl.when(e.valid)
        def _():
            for b in range(2):
                if e.gu:
                    wait(FG.at[e.slot, b], fin_send.at[b, e.slot])
                else:
                    wait(FD.at[e.slot, b], dfin_send.at[b, e.slot])

    streams = (gu_item, d_item)

    def send_terms(t):
        e = gu_item(t + 1, 0)
        @pl.when(e.valid)
        def _():
            remote(TS.at[1 - c, e.r], R.at[e.r], r_send, r_recv.at[e.r], sibling).start()
        f = d_item(t + 1, 0)
        @pl.when(f.sends)
        def _():
            for zz in range(nz):
                rs = pl.ds(pl.multiple_of(zz * crd + f.theirs * prow, 16), prow)
                remote(TD.at[f.layer, rs, :], RD.at[f.i, zz], rd_send, rd_recv.at[f.i], sibling).start()

    def terms_sent(t):
        e = gu_item(t + 1, 0)
        @pl.when(e.valid)
        def _():
            wait(R.at[e.r], r_send)
        f = d_item(t + 1, 0)
        @pl.when(f.sends)
        def _():
            wait(RD.at[f.i], rd_send)

    def reduce_step(t):
        terms_sent(t - 1)
        for which in streams:
            for s in range(half):
                stage_sent(which(t - LAG, s), s)
            last_sent(which(t - 1, half))
        for which in streams:
            last(which(t, half))
        for s in reversed(range(half)):
            for which in streams:
                e = which(t, s)
                if s == 0:
                    @pl.when(e.valid)
                    def _():
                        if e.gu:
                            wait(R.at[e.r], r_recv.at[e.r])
                        else:
                            wait(RD.at[e.i], rd_recv.at[e.i])
                stage(e, s)

    keep = (pltpu.make_async_copy(A, AH, load_sem.at[0]), pltpu.make_async_copy(AT, ATH, load_sem.at[1]))
    back = (pltpu.make_async_copy(AH, A, load_sem.at[0]), pltpu.make_async_copy(ATH, AT, load_sem.at[1]))

    def step(u, _):
        t = u - U1
        @pl.when(gathered(u) < gsteps)
        def _():
            def one(tg, _):
                gather_step(tg)
                return 0
            lax.fori_loop(gathered(u), gathered(u + 1), one, 0)
        @pl.when(t >= 0)
        def _():
            reduce_step(t)

        on, kind, j = work(u)
        slot = lax.rem(u, 2)
        @pl.when(u == UE - 1)
        def _():
            for m in range(2):
                down_rows(m, lax.rem(m + UF + CHUNKS, 2)).start()
        @pl.when(u == UE)
        def _():
            for m in range(2):
                kept(0, m, GUS, GUH, gu_sem).wait()
                kept(0, m, ACT, ACTH, act_sem).wait()
        def fetch():
            for there, copy in loads(u + 1):
                @pl.when(there)
                def _():
                    copy.start()
        pl.when(u != U1 - 1)(fetch)
        @pl.when(u == 2)
        def _():
            normalize(H, True)
            for copy in keep:
                copy.start()
        @pl.when(u == U1)
        def _():
            for copy in keep:
                copy.wait()
            after_forward()
        @pl.when(u == UB)
        def _():
            for copy in back:
                copy.start()
            for k in range(2):
                kept_act(k).start()
        @pl.when(u == UD)
        def _():
            between()
            for copy in back:
                copy.wait()
        for there, copy in loads(u):
            @pl.when(there)
            def _():
                copy.wait()
        @pl.when(on & (kind == 0))
        def _():
            forward(j, slot)
        @pl.when(on & (kind == 1))
        def _():
            second_layer(j, slot)
        @pl.when(on & (kind == 3))
        def _():
            first_layer(j, slot)
        @pl.when(t >= 0)
        def _():
            send_terms(t)
        @pl.when(on & (kind == 1))
        def _():
            down_gradient(1, j, slot)
        @pl.when((u >= UE) & (u < U1))
        def _():
            forward_down(u - UE)
        pl.when(u == U1 - 1)(fetch)
        @pl.when((u >= UB) & (u < UD))
        def _():
            input_gradient(u - UB)
        @pl.when((u >= UD) & (u < UC))
        def _():
            down_gradients(jnp.where(u == UD, 0, CHUNKS // 2), jnp.where(u == UD, CHUNKS // 2, CHUNKS))
        return 0

    lax.fori_loop(0, U1 + G0 + CHUNKS + SK * half + 1, step, 0)

    for i in range(1, n):
        remote(SQ, SQALL.at[me], sq_send, sq_recv, {"dp": lax.rem(me + i, n)}).start()
    for layer in range(2):
        wait(ggu.at[layer, 0], fin_recv.at[layer, 0])
        even = lax.rem(c + layer, 2) == 0
        @pl.when(even)
        def _():
            wait(gd.at[layer, pl.ds(0, PIECES // 2 * (prow // 2)), :], fin_recv.at[layer, 1])
        @pl.when(jnp.logical_not(even))
        def _():
            wait(gd.at[layer, pl.ds(0, (PIECES + 1) // 2 * (prow // 2)), :], fin_recv.at[layer, 1])
    wait(SQALL.at[pl.ds(0, n - 1)], sq_recv)
    acc = SQ[...]
    for i in range(1, n):
        acc = acc + SQALL[lax.rem(me + i, n)]
    sqo[0, 0] = jnp.sum(acc)
    wait(SQALL.at[pl.ds(0, n - 1)], sq_send)


def train(mesh, x, dy, w_gate, w_up, w_down):
    n = mesh.shape["dp"]
    nz = n // 2
    half = nz // 2
    tokens, d = x.shape
    layers, rgu, ff = w_gate.shape
    rd = ff // n
    cw = ff // CHUNKS
    prow = 2 * rd // PIECES
    items = (PIECES + 1) // 2
    V, S = pltpu.VMEM, pltpu.SemaphoreType.DMA
    shape = jax.ShapeDtypeStruct
    return pl.pallas_call(
        functools.partial(train_kernel, nz, math.isqrt(mesh.shape["rep"])),
        out_shape=(
            shape((layers, 2, rgu, ff), BF16), shape((layers, rd, d), BF16), shape((1, 1), F32),
            shape((layers, CHUNKS, 2, d, cw), BF16), shape((layers, ff, d), BF16),
            shape((CHUNKS, tokens, 2 * cw), F32), shape((CHUNKS, tokens, 2 * cw), BF16), shape((CHUNKS, tokens, cw), BF16),
            shape((tokens, d), BF16), shape((d, tokens), BF16),
        ),
        in_specs=[ANY] * 5,
        out_specs=(ANY, ANY, pl.BlockSpec(memory_space=pltpu.SMEM), ANY, ANY, ANY, ANY, ANY, ANY, ANY),
        scratch_shapes=[
            V((tokens, d), BF16), V((tokens, d), BF16), V((tokens, d), BF16), V((d, tokens), BF16), V((tokens, d), F32),
            V((2, d, 2 * cw), BF16), V((2, cw, d), BF16), V((2, tokens, 2 * cw), F32), V((2, tokens, 2 * cw), BF16), V((2, tokens, cw), BF16),
            V((2, CHUNKS, d, cw), BF16), V((CHUNKS, d, cw), BF16), V((layers, ff, d), BF16), V((2 * items, nz, prow, d), BF16),
            V((2, half + 1, SLOTS, 2 * rgu, cw), BF16), V((2, half + 1, DSLOTS, prow, d), BF16),
            V((SLOTS, 2, rgu, cw), BF16), V((DSLOTS, 2, prow // 2, d), BF16),
            V((8, 128), F32), V((n, 8, 128), F32), V((layers, CHUNKS, 2, rgu, cw), BF16), V((layers, rd, d), BF16),
            S((4,)), S((2, 5)), S((2,)), S((2,)), S((2,)), S((GSLOTS,)), S((2, half, RSLOTS)), S((GSLOTS,)), S((GSLOTS,)), S((GSLOTS,)),
            S, S((CHUNKS,)), S, S((2 * items,)), S((2, half, SLOTS)), S((2, half, SLOTS)), S((2, half, DSLOTS)), S((2, half, DSLOTS)),
            S((2, SLOTS)), S((2, DSLOTS)), S((layers, 2)), S, S,
        ],
        compiler_params=pltpu.CompilerParams(collective_id=0, has_side_effects=True, vmem_limit_bytes=63 * 2**20),
        name="train",
    )(x, dy, w_gate, w_up, w_down)


def adamw(w, m, v, g):
    m = 0.9 * m + 0.1 * g
    v = 0.95 * v + 0.05 * g * g
    step = m * lax.rsqrt(v + 1e-8) + 0.1 * w
    return (w - 0.02 * step).astype(BF16), m, v


def solution(mesh):
    n = mesh.shape["dp"]

    def step(x, dy, *arrays):
        weights, m, v = (arrays[i : i + 3] for i in (0, 3, 6))
        ggu, gd, squares = train(mesh, x[0], dy[0], *weights)[:3]
        gradients = [g.astype(F32) for g in (ggu[:, 0], ggu[:, 1], gd)]
        count = n * sum(g.size for g in gradients)
        factor = jnp.minimum(1.0, 0.5 * lax.rsqrt(squares[0, 0] / count + 1e-30))
        new = [adamw(w.astype(F32), m, v, g * factor) for w, m, v, g in zip(weights, m, v, gradients, strict=True)]
        return tuple(one[which] for which in range(3) for one in new)

    states, cut = P(("rep", "dp"), None, None), P(None, "dp", None)
    return jax.shard_map(
        step,
        mesh=mesh,
        in_specs=(states, states) + (cut,) * 9,
        out_specs=(P("rep", "dp", None),) * 9,
        check_vma=False,
    )
```

```python
import functools
import math

import jax
import jax.numpy as jnp
from jax import lax
from jax.experimental import pallas as pl
from jax.experimental.pallas import tpu as pltpu
from jax.sharding import PartitionSpec as P

MESH = pl.DeviceIdType.MESH
ANY = pl.BlockSpec(memory_space=pltpu.HBM)
F32, BF16 = jnp.float32, jnp.bfloat16
LAG = 3
SK = 2
DSLOTS = 8
SLOTS = 8
GSLOTS = 16
RSLOTS = 8
GPAR = 2
GDONE = 2
GSK = 2
DCH = 3
CHUNKS = 9
THREE = 3
PARTS = 2
PIECES = 9


def mm(a, b):
    return jnp.dot(a, b, preferred_element_type=F32)


def mm_nt(a, b):
    return lax.dot_general(a, b, (((1,), (1,)), ((), ())), preferred_element_type=F32)


def mm_tn(a, b):
    return lax.dot_general(a, b, (((0,), (0,)), ((), ())), preferred_element_type=F32)


def train_kernel(nz, ny, x, dy, wg, wu, wd, ggu, gd, sqo, WGU, WD, GUH, DGH, ACTH, AH, ATH,
                 H, DY, A, AT, DACC, WC, WDC, GUS, DGU, ACT, TS, R, TD, RD, BG, BD, FG, FD, SQ, SQALL, sgu, sd,
                 load_sem, w_sem, gu_sem, dg_sem, act_sem, own_sem, g_recv, g_sib, g_send, g_par,
                 r_send, r_recv, rd_send, rd_recv, ring_send, ring_recv, dring_send, dring_recv, fin_send, dfin_send, fin_recv, sq_send, sq_recv):
    me = lax.axis_index("dp")
    z, c = me // 2, me % 2
    n = 2 * nz
    half = nz // 2
    tokens, d = H.shape
    rgu = d // n
    cw = TS.shape[-1]
    ff = cw * CHUNKS
    rd = ff // n
    drow = rd // DCH
    crd = 2 * rd
    prow = crd // PIECES
    items = (PIECES + 1) // 2
    gper = DCH + CHUNKS
    gtotal = 2 * gper
    dhalf = (drow // 16 + 1) * 8
    gpar = GSK * half + GPAR
    gdone = gpar + GDONE
    UF = gdone + 1
    UE = UF + CHUNKS + DCH - 1
    U1 = UE + CHUNKS // THREE
    UB = U1 + CHUNKS
    UD = UB + CHUNKS // THREE
    UC = UD + 2
    G1, G0, D1 = 1, UC - U1 + 1, UC - U1 + 1 - items

    early = gper + DCH
    gsteps = early + 2 * (gtotal - 1 - early) + gdone + 1

    def gathered(u):
        return jnp.where(u < UE, u, UE + jnp.where(u < U1, lax.div(4 * (u - UE), 3), 4 * (U1 - UE) // 3 + 2 * (u - U1)))

    def started(t):
        late = t - early
        return (t >= 0) & ((late <= 0) | ((lax.rem(late, 2) == 0) & (t < gsteps - gdone))), jnp.where(late > 0, early + lax.div(late, 2), t)

    rep = lax.axis_index("rep")
    gx, gy = rep // ny, rep % ny
    diagonal = lax.rem(gx + gy, 2)
    beside_y = rep + 1 - 2 * lax.rem(gy, 2)
    beside_x = rep + ny * (1 - 2 * lax.rem(gx, 2))

    def dev(zz, cc):
        return {"dp": lax.rem(zz + nz, nz) * 2 + cc}

    up, down, sibling = dev(z + 1, c), dev(z - 1, c), dev(z, 1 - c)

    def remote(src, dst, s, r, to):
        return pltpu.make_async_remote_copy(src, dst, s, r, device_id=to, device_id_type=MESH)

    def wait(ref, sem):
        remote(ref, ref, sem, sem, sibling).wait_recv()

    first = [pltpu.make_async_copy(x, H, load_sem.at[0]), pltpu.make_async_copy(dy, DY, load_sem.at[1]), pltpu.make_async_copy(wd, sd, load_sem.at[2])]
    for cp in first:
        cp.start()
    for j in range(CHUNKS):
        for m, w in enumerate((wg, wu)):
            pltpu.make_async_copy(w.at[:, :, j * cw : (j + 1) * cw], sgu.at[:, j, m], load_sem.at[3]).start()

    barrier = pltpu.get_barrier_semaphore()
    for to in (up, down, sibling):
        pl.semaphore_signal(barrier, inc=1, device_id=to, device_id_type=MESH)
    for to in (beside_x, beside_y):
        pl.semaphore_signal(barrier, inc=1, device_id={"rep": to, "dp": me}, device_id_type=MESH)
    pl.semaphore_wait(barrier, 5)
    for cp in first:
        cp.wait()
    pltpu.make_async_copy(WGU.at[:, :, :, :rgu, :], sgu, load_sem.at[3]).wait()

    SQ[...] = jnp.zeros_like(SQ)

    def normalize(src, transposed):
        def rows(i, _):
            rs = pl.ds(pl.multiple_of(i * 128, 128), 128)
            wide = src[rs, :].astype(F32)
            a = (wide * lax.rsqrt(jnp.mean(wide * wide, -1, keepdims=True) + 1e-6)).astype(BF16)
            A[rs, :] = a
            if transposed:
                AT[:, rs] = a.T
            return 0
        lax.fori_loop(0, tokens // 128, rows, 0)

    def chunk(q):
        second = q >= gper
        r = jnp.where(second, q - gper, q)
        down = jnp.where(second, r, r - CHUNKS)
        is_down = (down >= 0) & (down < DCH)
        return jnp.where(second, 1, 0), is_down, jnp.where(is_down, down, jnp.where(second, r - DCH, r))

    def piece(q, blk, part, own, fn):
        layer, is_down, r = chunk(q)
        @pl.when(is_down)
        def _():
            def rows(first, size):
                here = pl.ds(pl.multiple_of(r * drow + first, 8), size)
                dst = WD.at[layer, pl.ds(pl.multiple_of(blk * rd + r * drow + first, 8), size), :]
                fn(sd.at[layer, here, :] if own else dst, dst)
            if part == 2:
                rows(0, drow)
            else:
                @pl.when(diagonal == part)
                def _():
                    rows(0, dhalf)
                @pl.when(diagonal != part)
                def _():
                    rows(dhalf, drow - dhalf)
        @pl.when(jnp.logical_not(is_down))
        def _():
            which = pl.ds(0, 2) if part == 2 else lax.rem(diagonal + part, 2)
            dst = WGU.at[layer, r, which, pl.ds(pl.multiple_of(blk * rgu, 8), rgu), :]
            fn(sgu.at[layer, r, which] if own else dst, dst)

    def block(zz):
        return jnp.where(zz >= nz, zz - nz, jnp.where(zz < 0, zz + nz, zz)) * 2 + c

    def to_sibling(q, src, dst):
        remote(src, dst, g_send.at[lax.rem(q, GSLOTS)], g_sib.at[lax.rem(q, GSLOTS)], sibling).start()

    def to_next(q, way, hop, src, dst):
        remote(src, dst, g_send.at[lax.rem(q, GSLOTS)], g_recv.at[hop - 1, lax.rem(q, RSLOTS)], (up, down)[way]).start()

    def to_beside(q, src, dst):
        to = jnp.where(lax.rem(q, 2) == 0, beside_y, beside_x)
        remote(src, dst, g_send.at[lax.rem(q, GSLOTS)], g_par.at[lax.rem(q, GSLOTS)], {"rep": to, "dp": me}).start()

    def come(q, part, count, sem):
        layer, is_down, _ = chunk(q)
        for first, rows in ((0, dhalf), (1, drow - dhalf)):
            @pl.when(is_down & (lax.rem(diagonal + part, 2) == first))
            def _():
                wait(WD.at[layer, pl.ds(0, count * rows), :], sem)
        @pl.when(jnp.logical_not(is_down))
        def _():
            wait(WGU.at[layer, 0, 0, pl.ds(0, count * rgu), :], sem)

    def gather_step(t):
        def start(q):
            def own(src, dst):
                to_next(q, 0, 1, src, dst)
                to_next(q, 1, 1, src, dst)
            piece(q, me, 0, True, own)
            def whole(src, dst):
                to_sibling(q, src, dst)
                pltpu.make_async_copy(src, dst, own_sem.at[lax.rem(q, GSLOTS)]).start()
            piece(q, me, 2, True, whole)
        there, first = started(t)
        pl.when(there)(lambda: start(first))
        for h in range(1, half + 1):
            there, q = started(t - GSK * h)
            @pl.when(there)
            def _():
                come(q, 0, 2 if h < half else 1, g_recv.at[h - 1, lax.rem(q, RSLOTS)])
                for way in (0, 1):
                    def go(src, dst):
                        if h < half - 1:
                            to_next(q, way, h + 1, src, dst)
                        elif h == half - 1:
                            @pl.when(lax.rem(q, 2) == way)
                            def _():
                                to_next(q, way, h + 1, src, dst)
                        to_beside(q, src, dst)
                    def take():
                        piece(q, block(z - h if way == 0 else z + h), 0, False, go)
                    if h < half:
                        take()
                    else:
                        pl.when(lax.rem(q, 2) == way)(take)
        there, q = started(t - gpar)
        @pl.when(there)
        def _():
            come(q, 1, nz - 1, g_par.at[lax.rem(q, GSLOTS)])
            for h in range(1, nz):
                piece(q, block(z + h), 2, False, lambda src, dst: to_sibling(q, src, dst))
        there, q = started(t - gdone)
        @pl.when(there)
        def _():
            layer, is_down, r = chunk(q)
            slot = lax.rem(q, GSLOTS)
            def waited(ref, sem):
                pltpu.make_async_copy(ref, ref, sem.at[slot]).wait()
            @pl.when(is_down)
            def _():
                rows = lambda k: WD.at[layer, pl.ds(0, k), :]
                waited(rows(drow), own_sem)
                waited(rows(nz * drow), g_sib)
                for mine in range(2):
                    @pl.when(diagonal == mine)
                    def _():
                        waited(rows(nz * drow + 2 * (nz - 1) * (drow - dhalf if mine else dhalf)), g_send)
            @pl.when(jnp.logical_not(is_down))
            def _():
                for k, sem in ((1, own_sem), (nz, g_sib), (2 * nz - 1, g_send)):
                    waited(WGU.at[layer, 0, :, pl.ds(0, k * rgu), :], sem)

    def work(u):
        ks = [u - first for first in (UF, U1, UC)]
        on = functools.reduce(jnp.logical_or, [(k >= 0) & (k < CHUNKS) for k in ks])
        pick = lambda a, b, c: jnp.where(u < UE, a, jnp.where(u < UC, b, c))
        return on, pick(0, 1, 3), pick(*ks)

    def loads(u):
        on, kind, j = work(u)
        layer = jnp.where((kind == 0) | (kind == 3), 0, 1)
        slot = lax.rem(u, 2)
        return (
            (on & (kind < 2), pltpu.make_async_copy(WGU.at[layer, j, 0], WC.at[slot, :, pl.ds(0, cw)], w_sem.at[slot, 0])),
            (on & (kind < 2), pltpu.make_async_copy(WGU.at[layer, j, 1], WC.at[slot, :, pl.ds(cw, cw)], w_sem.at[slot, 1])),
            (on & (kind > 0), pltpu.make_async_copy(WD.at[layer, pl.ds(pl.multiple_of(j * cw, 128), cw), :], WDC.at[slot], w_sem.at[slot, 2])),
            (on & (kind == 3), pltpu.make_async_copy(GUH.at[j], GUS.at[slot], w_sem.at[slot, 4])),
        )

    def kept(j, slot, buf, hbm, sem):
        return pltpu.make_async_copy(buf.at[slot], hbm.at[j], sem.at[slot])

    def forward(j, slot):
        @pl.when(j >= 2)
        def _():
            kept(j, slot, GUS, GUH, gu_sem).wait()
            kept(j, slot, ACT, ACTH, act_sem).wait()
        gu = mm(A[...], WC[slot])
        GUS[slot] = gu
        kept(j, slot, GUS, GUH, gu_sem).start()
        g, up = gu[:, :cw], gu[:, cw:]
        ACT[slot] = (g * jax.nn.sigmoid(g) * up).astype(BF16)
        kept(j, slot, ACT, ACTH, act_sem).start()

    def nth(m):
        return jnp.where(m < 2, CHUNKS - 2 + m, CHUNKS - 1 - m)

    def down_rows(m, slot):
        return pltpu.make_async_copy(WD.at[0, pl.ds(pl.multiple_of(nth(m) * cw, 128), cw), :], WDC.at[slot], w_sem.at[slot, 2])

    def forward_down(step):
        def one(i, _):
            m = THREE * step + i
            slot = lax.rem(m + UF + CHUNKS, 2)
            act = lambda k: pltpu.make_async_copy(ACTH.at[k], ACT.at[slot], act_sem.at[slot])
            down_rows(m, slot).wait()
            @pl.when(m >= 2)
            def _():
                act(0).wait()
            @pl.when(m == 0)
            def _():
                DACC[...] = jnp.zeros_like(DACC)
            DACC[...] += mm(ACT[slot], WDC[slot])
            @pl.when(m + 2 < CHUNKS)
            def _():
                down_rows(m + 2, slot).start()
                act(nth(m + 2)).start()
            return 0
        lax.fori_loop(0, THREE, one, 0)

    def down_gradient(layer, j, slot):
        TD[layer, pl.ds(pl.multiple_of(j * cw, 128), cw), :] = mm_tn(ACT[slot], DY[...]).astype(BF16)

    def kept_act(k):
        slot = lax.rem(k, 2)
        return pltpu.make_async_copy(ACTH.at[k], ACT.at[slot], act_sem.at[slot])

    def down_gradients(first, last):
        def one(k, _):
            kept_act(k).wait()
            down_gradient(0, k, lax.rem(k, 2))
            @pl.when(k + 2 < CHUNKS)
            def _():
                kept_act(k + 2).start()
            return 0
        lax.fori_loop(first, last, one, 0)

    def backward(products, j, slot, with_act):
        for first in range(0, tokens, tokens // PARTS):
            rs = pl.ds(first, tokens // PARTS)
            gu = products(rs)
            g, up = gu[:, :cw], gu[:, cw:]
            back = mm_nt(DY[rs, :], WDC[slot]).astype(BF16).astype(F32)
            sg = jax.nn.sigmoid(g)
            s = g * sg
            if with_act:
                ACT[slot, rs, :] = (s * up).astype(BF16)
            DGU[slot, rs, :cw] = (back * up * (sg + s * (1.0 - sg))).astype(BF16)
            DGU[slot, rs, cw:] = (back * s).astype(BF16)
        t = mm(AT[...], DGU[slot]).astype(BF16)
        TS[0, j] = t[:, :cw]
        TS[1, j] = t[:, cw:]

    def second_layer(j, slot):
        @pl.when(j >= 2)
        def _():
            kept(j, slot, DGU, DGH, dg_sem).wait()
        backward(lambda rs: mm(A[rs, :], WC[slot]), j, slot, True)
        @pl.when(j < CHUNKS - 2)
        def _():
            kept(j, slot, DGU, DGH, dg_sem).start()

    def first_layer(j, slot):
        backward(lambda rs: GUS[slot, rs, :], j, slot, False)

    def input_gradient(step):
        def again(k, slot):
            return (pltpu.make_async_copy(WGU.at[1, k, 0], WC.at[slot, :, pl.ds(0, cw)], w_sem.at[slot, 0]),
                    pltpu.make_async_copy(WGU.at[1, k, 1], WC.at[slot, :, pl.ds(cw, cw)], w_sem.at[slot, 1]),
                    pltpu.make_async_copy(DGH.at[k], DGU.at[slot], w_sem.at[slot, 3]))

        def one(i, _):
            m = THREE * step + i
            slot = lax.rem(m + U1 + CHUNKS, 2)
            @pl.when(m >= 2)
            def _():
                for copy in again(CHUNKS - 1 - m, slot):
                    copy.wait()
            @pl.when(m == 0)
            def _():
                DACC[...] = jnp.zeros_like(DACC)
            DACC[...] += mm_nt(DGU[slot], WC[slot])
            @pl.when(m + 2 < CHUNKS)
            def _():
                for copy in again(CHUNKS - 3 - m, slot):
                    copy.start()
            return 0
        lax.fori_loop(0, THREE, one, 0)

    def after_forward():
        def rows(i, _):
            rs = pl.ds(pl.multiple_of(i * 128, 128), 128)
            H[rs, :] = (H[rs, :].astype(F32) + DACC[rs, :].astype(BF16).astype(F32)).astype(BF16)
            return 0
        lax.fori_loop(0, tokens // 128, rows, 0)
        normalize(H, True)

    def between():
        def rows(i, _):
            rs = pl.ds(pl.multiple_of(i * 128, 128), 128)
            wide = H[rs, :].astype(F32)
            scale = lax.rsqrt(jnp.mean(wide * wide, -1, keepdims=True) + 1e-6)
            da = DACC[rs, :].astype(BF16).astype(F32)
            dh = scale * da - wide * (scale * scale * scale * jnp.mean(wide * da, -1, keepdims=True))
            DY[rs, :] = (DY[rs, :].astype(F32) + dh.astype(BF16).astype(F32)).astype(BF16)
            return 0
        lax.fori_loop(0, tokens // 128, rows, 0)

    class Item:
        pass

    def gu_item(t, s):
        e = Item()
        i = t - G1 - SK * s
        second = i < CHUNKS
        e.r = jnp.where(second, i, i - (G0 - G1))
        e.valid = (e.r >= 0) & (e.r < CHUNKS)
        e.layer = jnp.where(second, 1, 0)
        e.i, e.slot, e.odd, e.gu = i, lax.rem(i, SLOTS), lax.rem(e.r, 2), True
        e.buf, e.sent, e.come = BG, ring_send, ring_recv
        return e

    def d_item(t, s):
        e = Item()
        i = t - D1 - SK * s
        e.valid = (i >= 0) & (i < 2 * items)
        e.layer = jnp.where(i < items, 1, 0)
        k = i - (1 - e.layer) * items
        mine = jnp.where(e.layer == c, 0, 1)
        e.p, e.theirs = 2 * k + mine, 2 * k + 1 - mine
        e.sends, e.valid = e.valid & (e.theirs < PIECES), e.valid & (e.p < PIECES)
        e.i, e.slot, e.odd, e.gu = i, lax.rem(i, DSLOTS), lax.rem(k, 2), False
        e.buf, e.sent, e.come = BD, dring_send, dring_recv
        return e

    def terms(e, zz):
        if e.gu:
            rs = pl.ds(pl.multiple_of(zz * (2 * rgu), 16), 2 * rgu)
            return TS[c, e.r, rs, :].astype(F32) + R[e.r, rs, :].astype(F32)
        rs = pl.ds(pl.multiple_of(zz * crd + e.p * prow, 16), prow)
        return TD[e.layer, rs, :].astype(F32) + RD[e.i, zz].astype(F32)

    def around(zz):
        return jnp.where(zz >= nz, zz - nz, jnp.where(zz < 0, zz + nz, zz))

    def ring_copy(e, way, s):
        return remote(e.buf.at[way, s, e.slot], e.buf.at[way, s + 1, e.slot], e.sent.at[s, lax.rem(e.i, LAG + 1)], e.come.at[s, e.slot], (up, down)[way])

    def stage(e, s):
        def go(way):
            far = half - 1 - s + jnp.where(e.odd == way, 1, 0)
            t = terms(e, around(z + far if way == 0 else z - far))
            if s > 0:
                t = t + e.buf[way, s, e.slot].astype(F32)
            e.buf[way, s, e.slot] = t.astype(BF16)
            ring_copy(e, way, s).start()
        @pl.when(e.valid)
        def _():
            if s > 0:
                wait(e.buf.at[:, s, e.slot], e.come.at[s - 1, e.slot])
            if s < half - 1:
                go(0)
                go(1)
            else:
                for way in (0, 1):
                    @pl.when(e.odd == way)
                    def _():
                        go(way)

    def stage_sent(e, s):
        @pl.when(e.valid)
        def _():
            wait(e.buf.at[:, s, e.slot] if s < half - 1 else e.buf.at[0, s, e.slot], e.sent.at[s, lax.rem(e.i, LAG + 1)])

    def last(e):
        @pl.when(e.valid)
        def _():
            t = terms(e, z)
            wait(e.buf.at[0, half, e.slot], e.come.at[half - 1, e.slot])
            for way in (0, 1):
                t = t + e.buf[way, half - 1 + jnp.where(e.odd == way, 1, 0), e.slot].astype(F32)
            w = t.astype(BF16).astype(F32)
            sq = SQ[...]
            for a in range(w.shape[0] // 8):
                for b in range(w.shape[1] // 128):
                    v = w[8 * a : 8 * a + 8, 128 * b : 128 * b + 128]
                    sq = sq + v * v
            SQ[...] = sq
            out, rows = (FG, rgu) if e.gu else (FD, prow // 2)
            out[e.slot, 0] = w[:rows].astype(BF16)
            out[e.slot, 1] = w[rows:].astype(BF16)
            if e.gu:
                cs = pl.ds(pl.multiple_of(e.r * cw, 128), cw)
                pltpu.make_async_copy(FG.at[e.slot, c], ggu.at[e.layer, c, :, cs], fin_send.at[e.slot]).start()
                remote(FG.at[e.slot, 1 - c], ggu.at[e.layer, c, :, cs], fin_send.at[e.slot], fin_recv.at[e.layer, 0], sibling).start()
            else:
                for b in range(2):
                    k = 2 * e.p + b
                    theirs = k >= PIECES
                    row = jnp.where(theirs, k - PIECES, k) * (prow // 2)
                    dst = gd.at[e.layer, pl.ds(pl.multiple_of(row, 8), prow // 2), :]
                    owner = jnp.where(theirs, 1, 0)
                    @pl.when(owner == c)
                    def _():
                        pltpu.make_async_copy(FD.at[e.slot, b], dst, dfin_send.at[e.slot]).start()
                    @pl.when(owner != c)
                    def _():
                        remote(FD.at[e.slot, b], dst, dfin_send.at[e.slot], fin_recv.at[e.layer, 1], sibling).start()

    def last_sent(e):
        @pl.when(e.valid)
        def _():
            if e.gu:
                wait(FG.at[e.slot], fin_send.at[e.slot])
            else:
                wait(FD.at[e.slot], dfin_send.at[e.slot])

    streams = (gu_item, d_item)

    def send_terms(t):
        e = gu_item(t + 1, 0)
        @pl.when(e.valid)
        def _():
            remote(TS.at[1 - c, e.r], R.at[e.r], r_send, r_recv.at[e.r], sibling).start()
        f = d_item(t + 1, 0)
        @pl.when(f.sends)
        def _():
            for zz in range(nz):
                rs = pl.ds(pl.multiple_of(zz * crd + f.theirs * prow, 16), prow)
                remote(TD.at[f.layer, rs, :], RD.at[f.i, zz], rd_send, rd_recv.at[f.i], sibling).start()

    def terms_sent(t):
        e = gu_item(t + 1, 0)
        @pl.when(e.valid)
        def _():
            wait(R.at[e.r], r_send)
        f = d_item(t + 1, 0)
        @pl.when(f.sends)
        def _():
            wait(RD.at[f.i], rd_send)

    def reduce_step(t):
        terms_sent(t - 1)
        for which in streams:
            for s in range(half):
                stage_sent(which(t - LAG, s), s)
            last_sent(which(t - 1, half))
        for which in streams:
            last(which(t, half))
        for s in reversed(range(half)):
            for which in streams:
                e = which(t, s)
                if s == 0:
                    @pl.when(e.valid)
                    def _():
                        if e.gu:
                            wait(R.at[e.r], r_recv.at[e.r])
                        else:
                            wait(RD.at[e.i], rd_recv.at[e.i])
                stage(e, s)

    keep = (pltpu.make_async_copy(A, AH, load_sem.at[0]), pltpu.make_async_copy(AT, ATH, load_sem.at[1]))
    back = (pltpu.make_async_copy(AH, A, load_sem.at[0]), pltpu.make_async_copy(ATH, AT, load_sem.at[1]))

    def step(u, _):
        t = u - U1
        @pl.when(gathered(u) < gsteps)
        def _():
            def one(tg, _):
                gather_step(tg)
                return 0
            lax.fori_loop(gathered(u), gathered(u + 1), one, 0)
        @pl.when(t >= 0)
        def _():
            reduce_step(t)

        on, kind, j = work(u)
        slot = lax.rem(u, 2)
        @pl.when(u == UE - 1)
        def _():
            for m in range(2):
                down_rows(m, lax.rem(m + UF + CHUNKS, 2)).start()
        @pl.when(u == UE)
        def _():
            for m in range(2):
                kept(0, m, GUS, GUH, gu_sem).wait()
                kept(0, m, ACT, ACTH, act_sem).wait()
        def fetch():
            for there, copy in loads(u + 1):
                @pl.when(there)
                def _():
                    copy.start()
        pl.when(u != U1 - 1)(fetch)
        @pl.when(u == 1)
        def _():
            normalize(H, True)
            for copy in keep:
                copy.start()
        @pl.when(u == U1)
        def _():
            for copy in keep:
                copy.wait()
            after_forward()
        @pl.when(u == UB)
        def _():
            for copy in back:
                copy.start()
            for k in range(2):
                kept_act(k).start()
        @pl.when(u == UD)
        def _():
            between()
            for copy in back:
                copy.wait()
        for there, copy in loads(u):
            @pl.when(there)
            def _():
                copy.wait()
        @pl.when(on & (kind == 0))
        def _():
            forward(j, slot)
        @pl.when(on & (kind == 1))
        def _():
            second_layer(j, slot)
        @pl.when(on & (kind == 3))
        def _():
            first_layer(j, slot)
        @pl.when(t >= 0)
        def _():
            send_terms(t)
        @pl.when(on & (kind == 1))
        def _():
            down_gradient(1, j, slot)
        @pl.when((u >= UE) & (u < U1))
        def _():
            forward_down(u - UE)
        pl.when(u == U1 - 1)(fetch)
        @pl.when((u >= UB) & (u < UD))
        def _():
            input_gradient(u - UB)
        @pl.when((u >= UD) & (u < UC))
        def _():
            down_gradients(jnp.where(u == UD, 0, CHUNKS // 2), jnp.where(u == UD, CHUNKS // 2, CHUNKS))
        return 0

    lax.fori_loop(0, U1 + G0 + CHUNKS + SK * half + 1, step, 0)

    for i in range(1, n):
        remote(SQ, SQALL.at[me], sq_send, sq_recv, {"dp": lax.rem(me + i, n)}).start()
    for layer in range(2):
        wait(ggu.at[layer, 0], fin_recv.at[layer, 0])
        even = lax.rem(c + layer, 2) == 0
        @pl.when(even)
        def _():
            wait(gd.at[layer, pl.ds(0, PIECES // 2 * (prow // 2)), :], fin_recv.at[layer, 1])
        @pl.when(jnp.logical_not(even))
        def _():
            wait(gd.at[layer, pl.ds(0, (PIECES + 1) // 2 * (prow // 2)), :], fin_recv.at[layer, 1])
    wait(SQALL.at[pl.ds(0, n - 1)], sq_recv)
    acc = SQ[...]
    for i in range(1, n):
        acc = acc + SQALL[lax.rem(me + i, n)]
    sqo[0, 0] = jnp.sum(acc)
    wait(SQALL.at[pl.ds(0, n - 1)], sq_send)


def train(mesh, x, dy, w_gate, w_up, w_down):
    n = mesh.shape["dp"]
    nz = n // 2
    half = nz // 2
    tokens, d = x.shape
    layers, rgu, ff = w_gate.shape
    rd = ff // n
    cw = ff // CHUNKS
    prow = 2 * rd // PIECES
    items = (PIECES + 1) // 2
    V, S = pltpu.VMEM, pltpu.SemaphoreType.DMA
    shape = jax.ShapeDtypeStruct
    return pl.pallas_call(
        functools.partial(train_kernel, nz, math.isqrt(mesh.shape["rep"])),
        out_shape=(
            shape((layers, 2, rgu, ff), BF16), shape((layers, rd, d), BF16), shape((1, 1), F32),
            shape((layers, CHUNKS, 2, d, cw), BF16), shape((layers, ff, d), BF16),
            shape((CHUNKS, tokens, 2 * cw), F32), shape((CHUNKS, tokens, 2 * cw), BF16), shape((CHUNKS, tokens, cw), BF16),
            shape((tokens, d), BF16), shape((d, tokens), BF16),
        ),
        in_specs=[ANY] * 5,
        out_specs=(ANY, ANY, pl.BlockSpec(memory_space=pltpu.SMEM), ANY, ANY, ANY, ANY, ANY, ANY, ANY),
        scratch_shapes=[
            V((tokens, d), BF16), V((tokens, d), BF16), V((tokens, d), BF16), V((d, tokens), BF16), V((tokens, d), F32),
            V((2, d, 2 * cw), BF16), V((2, cw, d), BF16), V((2, tokens, 2 * cw), F32), V((2, tokens, 2 * cw), BF16), V((2, tokens, cw), BF16),
            V((2, CHUNKS, d, cw), BF16), V((CHUNKS, d, cw), BF16), V((layers, ff, d), BF16), V((2 * items, nz, prow, d), BF16),
            V((2, half + 1, SLOTS, 2 * rgu, cw), BF16), V((2, half + 1, DSLOTS, prow, d), BF16),
            V((SLOTS, 2, rgu, cw), BF16), V((DSLOTS, 2, prow // 2, d), BF16),
            V((8, 128), F32), V((n, 8, 128), F32), V((layers, CHUNKS, 2, rgu, cw), BF16), V((layers, rd, d), BF16),
            S((4,)), S((2, 5)), S((2,)), S((2,)), S((2,)), S((GSLOTS,)), S((half, RSLOTS)), S((GSLOTS,)), S((GSLOTS,)), S((GSLOTS,)),
            S, S((CHUNKS,)), S, S((2 * items,)), S((half, LAG + 1)), S((half, SLOTS)), S((half, LAG + 1)), S((half, DSLOTS)),
            S((SLOTS,)), S((DSLOTS,)), S((layers, 2)), S, S,
        ],
        compiler_params=pltpu.CompilerParams(collective_id=0, has_side_effects=True, vmem_limit_bytes=63 * 2**20),
        name="train",
    )(x, dy, w_gate, w_up, w_down)


def adamw(w, m, v, g):
    m = 0.9 * m + 0.1 * g
    v = 0.95 * v + 0.05 * g * g
    step = m * lax.rsqrt(v + 1e-8) + 0.1 * w
    return (w - 0.02 * step).astype(BF16), m, v


def solution(mesh):
    n = mesh.shape["dp"]

    def step(x, dy, *arrays):
        weights, m, v = (arrays[i : i + 3] for i in (0, 3, 6))
        ggu, gd, squares = train(mesh, x[0], dy[0], *weights)[:3]
        gradients = [g.astype(F32) for g in (ggu[:, 0], ggu[:, 1], gd)]
        count = n * sum(g.size for g in gradients)
        factor = jnp.minimum(1.0, 0.5 * lax.rsqrt(squares[0, 0] / count + 1e-30))
        new = [adamw(w.astype(F32), m, v, g * factor) for w, m, v, g in zip(weights, m, v, gradients, strict=True)]
        return tuple(one[which] for which in range(3) for one in new)

    states, cut = P(("rep", "dp"), None, None), P(None, "dp", None)
    return jax.shard_map(
        step,
        mesh=mesh,
        in_specs=(states, states) + (cut,) * 9,
        out_specs=(P("rep", "dp", None),) * 9,
        check_vma=False,
    )
```

```python
import functools
import math

import jax
import jax.numpy as jnp
from jax import lax
from jax.experimental import pallas as pl
from jax.experimental.pallas import tpu as pltpu
from jax.sharding import PartitionSpec as P

MESH = pl.DeviceIdType.MESH
ANY = pl.BlockSpec(memory_space=pltpu.HBM)
F32, BF16 = jnp.float32, jnp.bfloat16
LAG = 3
SK = 2
DSLOTS = 8
SLOTS = 8
GSLOTS = 16
RSLOTS = 8
GPAR = 2
GDONE = 2
GSK = 2
DCH = 3
CHUNKS = 9
THREE = 3
PARTS = 2
PIECES = 9


def mm(a, b):
    return jnp.dot(a, b, preferred_element_type=F32)


def mm_nt(a, b):
    return lax.dot_general(a, b, (((1,), (1,)), ((), ())), preferred_element_type=F32)


def mm_tn(a, b):
    return lax.dot_general(a, b, (((0,), (0,)), ((), ())), preferred_element_type=F32)


def train_kernel(nz, ny, x, dy, wg, wu, wd, ggu, gd, sqo, WGU, WD, GUH, DGH, ACTH, AH, ATH,
                 H, DY, A, AT, DACC, WC, WDC, GUS, DGU, ACT, TS, R, TD, RD, BG, BD, FG, FD, SQ, SQALL, sgu, sd,
                 load_sem, w_sem, gu_sem, dg_sem, act_sem, own_sem, g_recv, g_sib, g_send, g_par,
                 r_send, r_recv, rd_send, rd_recv, ring_send, ring_recv, dring_send, dring_recv, fin_send, dfin_send, fin_recv, sq_send, sq_recv):
    me = lax.axis_index("dp")
    z, c = me // 2, me % 2
    n = 2 * nz
    half = nz // 2
    tokens, d = H.shape
    rgu = d // n
    cw = TS.shape[-1]
    ff = cw * CHUNKS
    rd = ff // n
    drow = rd // DCH
    crd = 2 * rd
    prow = crd // PIECES
    items = (PIECES + 1) // 2
    gper = DCH + CHUNKS
    gtotal = 2 * gper
    dhalf = (drow // 16 + 1) * 8
    gpar = GSK * half + GPAR
    gdone = gpar + GDONE
    UF = gdone + 1
    UE = UF + CHUNKS + DCH - 1
    U1 = UE + CHUNKS // THREE
    UB = U1 + CHUNKS
    UD = UB + CHUNKS // THREE
    UC = UD + 2
    G1, G0, D1 = 1, UC - U1 + 1, UC - U1 + 1 - items

    early = gper + DCH
    gsteps = early + 2 * (gtotal - 1 - early) + gdone + 1

    def gathered(u):
        return jnp.where(u < UE, u, UE + jnp.where(u < U1, lax.div(4 * (u - UE), 3), 4 * (U1 - UE) // 3 + 2 * (u - U1)))

    def started(t):
        late = t - early
        return (t >= 0) & ((late <= 0) | ((lax.rem(late, 2) == 0) & (t < gsteps - gdone))), jnp.where(late > 0, early + lax.div(late, 2), t)

    rep = lax.axis_index("rep")
    gx, gy = rep // ny, rep % ny
    diagonal = lax.rem(gx + gy, 2)
    beside_y = rep + 1 - 2 * lax.rem(gy, 2)
    beside_x = rep + ny * (1 - 2 * lax.rem(gx, 2))

    def dev(zz, cc):
        return {"dp": lax.rem(zz + nz, nz) * 2 + cc}

    up, down, sibling = dev(z + 1, c), dev(z - 1, c), dev(z, 1 - c)

    def remote(src, dst, s, r, to):
        return pltpu.make_async_remote_copy(src, dst, s, r, device_id=to, device_id_type=MESH)

    def wait(ref, sem):
        remote(ref, ref, sem, sem, sibling).wait_recv()

    first = [pltpu.make_async_copy(x, H, load_sem.at[0]), pltpu.make_async_copy(dy, DY, load_sem.at[1]), pltpu.make_async_copy(wd, sd, load_sem.at[2])]
    for cp in first:
        cp.start()
    for j in range(CHUNKS):
        for m, w in enumerate((wg, wu)):
            pltpu.make_async_copy(w.at[:, :, j * cw : (j + 1) * cw], sgu.at[:, j, m], load_sem.at[3]).start()

    barrier = pltpu.get_barrier_semaphore()
    for to in (up, down, sibling):
        pl.semaphore_signal(barrier, inc=1, device_id=to, device_id_type=MESH)
    for to in (beside_x, beside_y):
        pl.semaphore_signal(barrier, inc=1, device_id={"rep": to, "dp": me}, device_id_type=MESH)
    pl.semaphore_wait(barrier, 5)
    for cp in first:
        cp.wait()
    pltpu.make_async_copy(WGU.at[:, :, :, :rgu, :], sgu, load_sem.at[3]).wait()

    SQ[...] = jnp.zeros_like(SQ)

    def normalize(src, transposed):
        def rows(i, _):
            rs = pl.ds(pl.multiple_of(i * 128, 128), 128)
            wide = src[rs, :].astype(F32)
            a = (wide * lax.rsqrt(jnp.mean(wide * wide, -1, keepdims=True) + 1e-6)).astype(BF16)
            A[rs, :] = a
            if transposed:
                AT[:, rs] = a.T
            return 0
        lax.fori_loop(0, tokens // 128, rows, 0)

    def chunk(q):
        second = q >= gper
        r = jnp.where(second, q - gper, q)
        down = jnp.where(second, r, r - CHUNKS)
        is_down = (down >= 0) & (down < DCH)
        return jnp.where(second, 1, 0), is_down, jnp.where(is_down, down, jnp.where(second, r - DCH, r))

    def piece(q, blk, part, own, fn):
        layer, is_down, r = chunk(q)
        @pl.when(is_down)
        def _():
            def rows(first, size):
                here = pl.ds(pl.multiple_of(r * drow + first, 8), size)
                dst = WD.at[layer, pl.ds(pl.multiple_of(blk * rd + r * drow + first, 8), size), :]
                fn(sd.at[layer, here, :] if own else dst, dst)
            if part == 2:
                rows(0, drow)
            else:
                @pl.when(diagonal == part)
                def _():
                    rows(0, dhalf)
                @pl.when(diagonal != part)
                def _():
                    rows(dhalf, drow - dhalf)
        @pl.when(jnp.logical_not(is_down))
        def _():
            which = pl.ds(0, 2) if part == 2 else lax.rem(diagonal + part, 2)
            dst = WGU.at[layer, r, which, pl.ds(pl.multiple_of(blk * rgu, 8), rgu), :]
            fn(sgu.at[layer, r, which] if own else dst, dst)

    def block(zz):
        return jnp.where(zz >= nz, zz - nz, jnp.where(zz < 0, zz + nz, zz)) * 2 + c

    def to_sibling(q, src, dst):
        remote(src, dst, g_send.at[lax.rem(q, GSLOTS)], g_sib.at[lax.rem(q, GSLOTS)], sibling).start()

    def to_next(q, way, hop, src, dst):
        remote(src, dst, g_send.at[lax.rem(q, GSLOTS)], g_recv.at[hop - 1, lax.rem(q, RSLOTS)], (up, down)[way]).start()

    def to_beside(q, src, dst):
        to = jnp.where(lax.rem(q, 2) == 0, beside_y, beside_x)
        remote(src, dst, g_send.at[lax.rem(q, GSLOTS)], g_par.at[lax.rem(q, GSLOTS)], {"rep": to, "dp": me}).start()

    def come(q, part, count, sem):
        layer, is_down, _ = chunk(q)
        for first, rows in ((0, dhalf), (1, drow - dhalf)):
            @pl.when(is_down & (lax.rem(diagonal + part, 2) == first))
            def _():
                wait(WD.at[layer, pl.ds(0, count * rows), :], sem)
        @pl.when(jnp.logical_not(is_down))
        def _():
            wait(WGU.at[layer, 0, 0, pl.ds(0, count * rgu), :], sem)

    def gather_step(t):
        def start(q):
            def own(src, dst):
                to_next(q, 0, 1, src, dst)
                to_next(q, 1, 1, src, dst)
            piece(q, me, 0, True, own)
            def whole(src, dst):
                to_sibling(q, src, dst)
                pltpu.make_async_copy(src, dst, own_sem.at[lax.rem(q, GSLOTS)]).start()
            piece(q, me, 2, True, whole)
        there, first = started(t)
        pl.when(there)(lambda: start(first))
        for h in range(1, half + 1):
            there, q = started(t - GSK * h)
            @pl.when(there)
            def _():
                come(q, 0, 2 if h < half else 1, g_recv.at[h - 1, lax.rem(q, RSLOTS)])
                for way in (0, 1):
                    def go(src, dst):
                        if h < half - 1:
                            to_next(q, way, h + 1, src, dst)
                        elif h == half - 1:
                            @pl.when(lax.rem(q, 2) == way)
                            def _():
                                to_next(q, way, h + 1, src, dst)
                        to_beside(q, src, dst)
                    def take():
                        piece(q, block(z - h if way == 0 else z + h), 0, False, go)
                    if h < half:
                        take()
                    else:
                        pl.when(lax.rem(q, 2) == way)(take)
        there, q = started(t - gpar)
        @pl.when(there)
        def _():
            come(q, 1, nz - 1, g_par.at[lax.rem(q, GSLOTS)])
            for h in range(1, nz):
                piece(q, block(z + h), 2, False, lambda src, dst: to_sibling(q, src, dst))
        there, q = started(t - gdone)
        @pl.when(there)
        def _():
            layer, is_down, r = chunk(q)
            slot = lax.rem(q, GSLOTS)
            def waited(ref, sem):
                pltpu.make_async_copy(ref, ref, sem.at[slot]).wait()
            @pl.when(is_down)
            def _():
                rows = lambda k: WD.at[layer, pl.ds(0, k), :]
                waited(rows(drow), own_sem)
                waited(rows(nz * drow), g_sib)
                for mine in range(2):
                    @pl.when(diagonal == mine)
                    def _():
                        waited(rows(nz * drow + 2 * (nz - 1) * (drow - dhalf if mine else dhalf)), g_send)
            @pl.when(jnp.logical_not(is_down))
            def _():
                for k, sem in ((1, own_sem), (nz, g_sib), (2 * nz - 1, g_send)):
                    waited(WGU.at[layer, 0, :, pl.ds(0, k * rgu), :], sem)

    def work(u):
        ks = [u - first for first in (UF, U1, UC)]
        on = functools.reduce(jnp.logical_or, [(k >= 0) & (k < CHUNKS) for k in ks])
        pick = lambda a, b, c: jnp.where(u < UE, a, jnp.where(u < UC, b, c))
        return on, pick(0, 1, 3), pick(*ks)

    def loads(u):
        on, kind, j = work(u)
        layer = jnp.where((kind == 0) | (kind == 3), 0, 1)
        slot = lax.rem(u, 2)
        return (
            (on & (kind < 2), pltpu.make_async_copy(WGU.at[layer, j, 0], WC.at[slot, :, pl.ds(0, cw)], w_sem.at[slot, 0])),
            (on & (kind < 2), pltpu.make_async_copy(WGU.at[layer, j, 1], WC.at[slot, :, pl.ds(cw, cw)], w_sem.at[slot, 1])),
            (on & (kind > 0), pltpu.make_async_copy(WD.at[layer, pl.ds(pl.multiple_of(j * cw, 128), cw), :], WDC.at[slot], w_sem.at[slot, 2])),
            (on & (kind == 3), pltpu.make_async_copy(GUH.at[j], GUS.at[slot], w_sem.at[slot, 4])),
        )

    def kept(j, slot, buf, hbm, sem):
        return pltpu.make_async_copy(buf.at[slot], hbm.at[j], sem.at[slot])

    def forward(j, slot):
        @pl.when(j >= 2)
        def _():
            kept(j, slot, GUS, GUH, gu_sem).wait()
            kept(j, slot, ACT, ACTH, act_sem).wait()
        gu = mm(A[...], WC[slot])
        GUS[slot] = gu
        kept(j, slot, GUS, GUH, gu_sem).start()
        g, up = gu[:, :cw], gu[:, cw:]
        ACT[slot] = (g * jax.nn.sigmoid(g) * up).astype(BF16)
        kept(j, slot, ACT, ACTH, act_sem).start()

    def nth(m):
        return jnp.where(m < 2, CHUNKS - 2 + m, CHUNKS - 1 - m)

    def down_rows(m, slot):
        return pltpu.make_async_copy(WD.at[0, pl.ds(pl.multiple_of(nth(m) * cw, 128), cw), :], WDC.at[slot], w_sem.at[slot, 2])

    def forward_down(step):
        def one(i, _):
            m = THREE * step + i
            slot = lax.rem(m + UF + CHUNKS, 2)
            act = lambda k: pltpu.make_async_copy(ACTH.at[k], ACT.at[slot], act_sem.at[slot])
            down_rows(m, slot).wait()
            @pl.when(m >= 2)
            def _():
                act(0).wait()
            @pl.when(m == 0)
            def _():
                DACC[...] = jnp.zeros_like(DACC)
            DACC[...] += mm(ACT[slot], WDC[slot])
            @pl.when(m + 2 < CHUNKS)
            def _():
                down_rows(m + 2, slot).start()
                act(nth(m + 2)).start()
            return 0
        lax.fori_loop(0, THREE, one, 0)

    def down_gradient(layer, j, slot):
        TD[layer, pl.ds(pl.multiple_of(j * cw, 128), cw), :] = mm_tn(ACT[slot], DY[...]).astype(BF16)

    def kept_act(k):
        slot = lax.rem(k, 2)
        return pltpu.make_async_copy(ACTH.at[k], ACT.at[slot], act_sem.at[slot])

    def down_gradients(first, last):
        def one(k, _):
            kept_act(k).wait()
            down_gradient(0, k, lax.rem(k, 2))
            @pl.when(k + 2 < CHUNKS)
            def _():
                kept_act(k + 2).start()
            return 0
        lax.fori_loop(first, last, one, 0)

    def backward(products, j, slot, with_act):
        for first in range(0, tokens, tokens // PARTS):
            rs = pl.ds(first, tokens // PARTS)
            gu = products(rs)
            g, up = gu[:, :cw], gu[:, cw:]
            back = mm_nt(DY[rs, :], WDC[slot]).astype(BF16).astype(F32)
            sg = jax.nn.sigmoid(g)
            s = g * sg
            if with_act:
                ACT[slot, rs, :] = (s * up).astype(BF16)
            DGU[slot, rs, :cw] = (back * up * (sg + s * (1.0 - sg))).astype(BF16)
            DGU[slot, rs, cw:] = (back * s).astype(BF16)
        t = mm(AT[...], DGU[slot]).astype(BF16)
        TS[0, j] = t[:, :cw]
        TS[1, j] = t[:, cw:]

    def second_layer(j, slot):
        @pl.when(j >= 2)
        def _():
            kept(j, slot, DGU, DGH, dg_sem).wait()
        backward(lambda rs: mm(A[rs, :], WC[slot]), j, slot, True)
        @pl.when(j < CHUNKS - 2)
        def _():
            kept(j, slot, DGU, DGH, dg_sem).start()

    def first_layer(j, slot):
        backward(lambda rs: GUS[slot, rs, :], j, slot, False)

    def input_gradient(step):
        def again(k, slot):
            return (pltpu.make_async_copy(WGU.at[1, k, 0], WC.at[slot, :, pl.ds(0, cw)], w_sem.at[slot, 0]),
                    pltpu.make_async_copy(WGU.at[1, k, 1], WC.at[slot, :, pl.ds(cw, cw)], w_sem.at[slot, 1]),
                    pltpu.make_async_copy(DGH.at[k], DGU.at[slot], w_sem.at[slot, 3]))

        def one(i, _):
            m = THREE * step + i
            slot = lax.rem(m + U1 + CHUNKS, 2)
            @pl.when(m >= 2)
            def _():
                for copy in again(CHUNKS - 1 - m, slot):
                    copy.wait()
            @pl.when(m == 0)
            def _():
                DACC[...] = jnp.zeros_like(DACC)
            DACC[...] += mm_nt(DGU[slot], WC[slot])
            @pl.when(m + 2 < CHUNKS)
            def _():
                for copy in again(CHUNKS - 3 - m, slot):
                    copy.start()
            return 0
        lax.fori_loop(0, THREE, one, 0)

    def after_forward():
        def rows(i, _):
            rs = pl.ds(pl.multiple_of(i * 128, 128), 128)
            H[rs, :] = (H[rs, :].astype(F32) + DACC[rs, :].astype(BF16).astype(F32)).astype(BF16)
            return 0
        lax.fori_loop(0, tokens // 128, rows, 0)
        normalize(H, True)

    def between():
        def rows(i, _):
            rs = pl.ds(pl.multiple_of(i * 128, 128), 128)
            wide = H[rs, :].astype(F32)
            scale = lax.rsqrt(jnp.mean(wide * wide, -1, keepdims=True) + 1e-6)
            da = DACC[rs, :].astype(BF16).astype(F32)
            dh = scale * da - wide * (scale * scale * scale * jnp.mean(wide * da, -1, keepdims=True))
            DY[rs, :] = (DY[rs, :].astype(F32) + dh.astype(BF16).astype(F32)).astype(BF16)
            return 0
        lax.fori_loop(0, tokens // 128, rows, 0)

    class Item:
        pass

    def gu_item(t, s):
        e = Item()
        i = t - G1 - SK * s
        second = i < CHUNKS
        e.r = jnp.where(second, i, i - (G0 - G1))
        e.valid = (e.r >= 0) & (e.r < CHUNKS)
        e.layer = jnp.where(second, 1, 0)
        e.i, e.slot, e.odd, e.gu = i, lax.rem(i, SLOTS), lax.rem(e.r, 2), True
        e.buf, e.sent, e.come = BG, ring_send, ring_recv
        return e

    def d_item(t, s):
        e = Item()
        i = t - D1 - SK * s
        e.valid = (i >= 0) & (i < 2 * items)
        e.layer = jnp.where(i < items, 1, 0)
        k = i - (1 - e.layer) * items
        mine = jnp.where(e.layer == c, 0, 1)
        e.p, e.theirs = 2 * k + mine, 2 * k + 1 - mine
        e.sends, e.valid = e.valid & (e.theirs < PIECES), e.valid & (e.p < PIECES)
        e.i, e.slot, e.odd, e.gu = i, lax.rem(i, DSLOTS), lax.rem(k, 2), False
        e.buf, e.sent, e.come = BD, dring_send, dring_recv
        return e

    def terms(e, zz):
        if e.gu:
            rs = pl.ds(pl.multiple_of(zz * (2 * rgu), 16), 2 * rgu)
            return TS[c, e.r, rs, :].astype(F32) + R[e.r, rs, :].astype(F32)
        rs = pl.ds(pl.multiple_of(zz * crd + e.p * prow, 16), prow)
        return TD[e.layer, rs, :].astype(F32) + RD[e.i, zz].astype(F32)

    def around(zz):
        return jnp.where(zz >= nz, zz - nz, jnp.where(zz < 0, zz + nz, zz))

    def ring_copy(e, way, s):
        return remote(e.buf.at[way, s, e.slot], e.buf.at[way, s + 1, e.slot], e.sent.at[s, lax.rem(e.i, LAG + 1)], e.come.at[s, e.slot], (up, down)[way])

    def stage(e, s):
        def go(way):
            far = half - 1 - s + jnp.where(e.odd == way, 1, 0)
            t = terms(e, around(z + far if way == 0 else z - far))
            if s > 0:
                t = t + e.buf[way, s, e.slot].astype(F32)
            e.buf[way, s, e.slot] = t.astype(BF16)
            ring_copy(e, way, s).start()
        @pl.when(e.valid)
        def _():
            if s > 0:
                wait(e.buf.at[:, s, e.slot], e.come.at[s - 1, e.slot])
            if s < half - 1:
                go(0)
                go(1)
            else:
                for way in (0, 1):
                    @pl.when(e.odd == way)
                    def _():
                        go(way)

    def stage_sent(e, s):
        @pl.when(e.valid)
        def _():
            wait(e.buf.at[:, s, e.slot] if s < half - 1 else e.buf.at[0, s, e.slot], e.sent.at[s, lax.rem(e.i, LAG + 1)])

    def last(e):
        @pl.when(e.valid)
        def _():
            t = terms(e, z)
            wait(e.buf.at[0, half, e.slot], e.come.at[half - 1, e.slot])
            for way in (0, 1):
                t = t + e.buf[way, half - 1 + jnp.where(e.odd == way, 1, 0), e.slot].astype(F32)
            w = t.astype(BF16).astype(F32)
            sq = SQ[...]
            for a in range(w.shape[0] // 8):
                for b in range(w.shape[1] // 128):
                    v = w[8 * a : 8 * a + 8, 128 * b : 128 * b + 128]
                    sq = sq + v * v
            SQ[...] = sq
            out, rows = (FG, rgu) if e.gu else (FD, prow // 2)
            out[e.slot, 0] = w[:rows].astype(BF16)
            out[e.slot, 1] = w[rows:].astype(BF16)
            if e.gu:
                cs = pl.ds(pl.multiple_of(e.r * cw, 128), cw)
                pltpu.make_async_copy(FG.at[e.slot, c], ggu.at[e.layer, c, :, cs], fin_send.at[e.slot]).start()
                remote(FG.at[e.slot, 1 - c], ggu.at[e.layer, c, :, cs], fin_send.at[e.slot], fin_recv.at[e.layer, 0], sibling).start()
            else:
                for b in range(2):
                    k = 2 * e.p + b
                    theirs = k >= PIECES
                    row = jnp.where(theirs, k - PIECES, k) * (prow // 2)
                    dst = gd.at[e.layer, pl.ds(pl.multiple_of(row, 8), prow // 2), :]
                    owner = jnp.where(theirs, 1, 0)
                    @pl.when(owner == c)
                    def _():
                        pltpu.make_async_copy(FD.at[e.slot, b], dst, dfin_send.at[e.slot]).start()
                    @pl.when(owner != c)
                    def _():
                        remote(FD.at[e.slot, b], dst, dfin_send.at[e.slot], fin_recv.at[e.layer, 1], sibling).start()

    def last_sent(e):
        @pl.when(e.valid)
        def _():
            if e.gu:
                wait(FG.at[e.slot], fin_send.at[e.slot])
            else:
                wait(FD.at[e.slot], dfin_send.at[e.slot])

    streams = (gu_item, d_item)

    def send_terms(t):
        e = gu_item(t + 1, 0)
        @pl.when(e.valid)
        def _():
            remote(TS.at[1 - c, e.r], R.at[e.r], r_send, r_recv.at[e.r], sibling).start()
        f = d_item(t + 1, 0)
        @pl.when(f.sends)
        def _():
            for zz in range(nz):
                rs = pl.ds(pl.multiple_of(zz * crd + f.theirs * prow, 16), prow)
                remote(TD.at[f.layer, rs, :], RD.at[f.i, zz], rd_send, rd_recv.at[f.i], sibling).start()

    def terms_sent(t):
        e = gu_item(t + 1, 0)
        @pl.when(e.valid)
        def _():
            wait(R.at[e.r], r_send)
        f = d_item(t + 1, 0)
        @pl.when(f.sends)
        def _():
            wait(RD.at[f.i], rd_send)

    def reduce_step(t):
        terms_sent(t - 1)
        for which in streams:
            for s in range(half):
                stage_sent(which(t - LAG, s), s)
            last_sent(which(t - 1, half))
        for which in streams:
            last(which(t, half))
        for s in reversed(range(half)):
            for which in streams:
                e = which(t, s)
                if s == 0:
                    @pl.when(e.valid)
                    def _():
                        if e.gu:
                            wait(R.at[e.r], r_recv.at[e.r])
                        else:
                            wait(RD.at[e.i], rd_recv.at[e.i])
                stage(e, s)

    keep = (pltpu.make_async_copy(A, AH, load_sem.at[0]), pltpu.make_async_copy(AT, ATH, load_sem.at[1]))
    back = (pltpu.make_async_copy(AH, A, load_sem.at[0]), pltpu.make_async_copy(ATH, AT, load_sem.at[1]))

    def step(u, _):
        t = u - U1
        @pl.when(gathered(u) < gsteps)
        def _():
            def one(tg, _):
                gather_step(tg)
                return 0
            lax.fori_loop(gathered(u), gathered(u + 1), one, 0)
        @pl.when(t >= 0)
        def _():
            reduce_step(t)

        on, kind, j = work(u)
        slot = lax.rem(u, 2)
        @pl.when(u == UE - 1)
        def _():
            for m in range(2):
                down_rows(m, lax.rem(m + UF + CHUNKS, 2)).start()
        @pl.when(u == UE)
        def _():
            for m in range(2):
                kept(0, m, GUS, GUH, gu_sem).wait()
                kept(0, m, ACT, ACTH, act_sem).wait()
        def fetch():
            for there, copy in loads(u + 1):
                @pl.when(there)
                def _():
                    copy.start()
        pl.when(u != U1 - 1)(fetch)
        @pl.when(u == 1)
        def _():
            normalize(H, True)
            for copy in keep:
                copy.start()
        @pl.when(u == U1)
        def _():
            for copy in keep:
                copy.wait()
            after_forward()
        @pl.when(u == UB)
        def _():
            for copy in back:
                copy.start()
            for k in range(2):
                kept_act(k).start()
        @pl.when(u == UD)
        def _():
            between()
            for copy in back:
                copy.wait()
        for there, copy in loads(u):
            @pl.when(there)
            def _():
                copy.wait()
        @pl.when(on & (kind == 0))
        def _():
            forward(j, slot)
        @pl.when(on & (kind == 1))
        def _():
            second_layer(j, slot)
        @pl.when(on & (kind == 3))
        def _():
            first_layer(j, slot)
        @pl.when(t >= 0)
        def _():
            send_terms(t)
        @pl.when(on & (kind == 1))
        def _():
            down_gradient(1, j, slot)
        @pl.when((u >= UE) & (u < U1))
        def _():
            forward_down(u - UE)
        pl.when(u == U1 - 1)(fetch)
        @pl.when((u >= UB) & (u < UD))
        def _():
            input_gradient(u - UB)
        @pl.when((u >= UD) & (u < UC))
        def _():
            down_gradients(jnp.where(u == UD, 0, CHUNKS // 2), jnp.where(u == UD, CHUNKS // 2, CHUNKS))
        return 0

    lax.fori_loop(0, U1 + G0 + CHUNKS + SK * half + 1, step, 0)

    for i in range(1, n):
        remote(SQ, SQALL.at[me], sq_send, sq_recv, {"dp": lax.rem(me + i, n)}).start()
    for layer in range(2):
        wait(ggu.at[layer, 0], fin_recv.at[layer, 0])
        even = lax.rem(c + layer, 2) == 0
        @pl.when(even)
        def _():
            wait(gd.at[layer, pl.ds(0, PIECES // 2 * (prow // 2)), :], fin_recv.at[layer, 1])
        @pl.when(jnp.logical_not(even))
        def _():
            wait(gd.at[layer, pl.ds(0, (PIECES + 1) // 2 * (prow // 2)), :], fin_recv.at[layer, 1])
    wait(SQALL.at[pl.ds(0, n - 1)], sq_recv)
    acc = SQ[...]
    for i in range(1, n):
        acc = acc + SQALL[lax.rem(me + i, n)]
    sqo[0, 0] = jnp.sum(acc)
    wait(SQALL.at[pl.ds(0, n - 1)], sq_send)


def train(mesh, x, dy, w_gate, w_up, w_down):
    n = mesh.shape["dp"]
    nz = n // 2
    half = nz // 2
    tokens, d = x.shape
    layers, rgu, ff = w_gate.shape
    rd = ff // n
    cw = ff // CHUNKS
    prow = 2 * rd // PIECES
    items = (PIECES + 1) // 2
    V, S = pltpu.VMEM, pltpu.SemaphoreType.DMA
    shape = jax.ShapeDtypeStruct
    return pl.pallas_call(
        functools.partial(train_kernel, nz, math.isqrt(mesh.shape["rep"])),
        out_shape=(
            shape((layers, 2, rgu, ff), BF16), shape((layers, rd, d), BF16), shape((1, 1), F32),
            shape((layers, CHUNKS, 2, d, cw), BF16), shape((layers, ff, d), BF16),
            shape((CHUNKS, tokens, 2 * cw), F32), shape((CHUNKS, tokens, 2 * cw), BF16), shape((CHUNKS, tokens, cw), BF16),
            shape((tokens, d), BF16), shape((d, tokens), BF16),
        ),
        in_specs=[ANY] * 5,
        out_specs=(ANY, ANY, pl.BlockSpec(memory_space=pltpu.SMEM), ANY, ANY, ANY, ANY, ANY, ANY, ANY),
        scratch_shapes=[
            V((tokens, d), BF16), V((tokens, d), BF16), V((tokens, d), BF16), V((d, tokens), BF16), V((tokens, d), F32),
            V((2, d, 2 * cw), BF16), V((2, cw, d), BF16), V((2, tokens, 2 * cw), F32), V((2, tokens, 2 * cw), BF16), V((2, tokens, cw), BF16),
            V((2, CHUNKS, d, cw), BF16), V((CHUNKS, d, cw), BF16), V((layers, ff, d), BF16), V((2 * items, nz, prow, d), BF16),
            V((2, half + 1, SLOTS, 2 * rgu, cw), BF16), V((2, half + 1, DSLOTS, prow, d), BF16),
            V((SLOTS, 2, rgu, cw), BF16), V((DSLOTS, 2, prow // 2, d), BF16),
            V((8, 128), F32), V((n, 8, 128), F32), V((layers, CHUNKS, 2, rgu, cw), BF16), V((layers, rd, d), BF16),
            S((4,)), S((2, 5)), S((2,)), S((2,)), S((2,)), S((GSLOTS,)), S((half, RSLOTS)), S((GSLOTS,)), S((GSLOTS,)), S((GSLOTS,)),
            S, S((CHUNKS,)), S, S((2 * items,)), S((half, LAG + 1)), S((half, SLOTS)), S((half, LAG + 1)), S((half, DSLOTS)),
            S((SLOTS,)), S((DSLOTS,)), S((layers, 2)), S, S,
        ],
        compiler_params=pltpu.CompilerParams(collective_id=0, has_side_effects=True, vmem_limit_bytes=63 * 2**20),
        name="train",
    )(x, dy, w_gate, w_up, w_down)


def adamw(w, m, v, g):
    m = 0.9 * m + 0.1 * g
    v = 0.95 * v + 0.05 * g * g
    step = m * lax.rsqrt(v + 1e-8) + 0.1 * w
    return (w - 0.02 * step).astype(BF16), m, v


def update_kernel(count, squares, ggu, gd, *refs):
    ins, outs = refs[:9], refs[9:]
    mean = jnp.full((8, 128), squares[0, 0] * (1.0 / count), F32)
    factor = jnp.minimum(1.0, 0.5 * lax.rsqrt(mean + 1e-30))[:1, :1]
    for i, g in enumerate((ggu[0, 0], ggu[0, 1], gd[0])):
        w, m, v = (ins[i + 3 * k][0].astype(F32) for k in range(3))
        for k, one in enumerate(adamw(w, m, v, g.astype(F32) * factor)):
            outs[i + 3 * k][0] = one


def update(n, squares, ggu, gd, arrays):
    layers, _, rgu, ff = ggu.shape
    rd, d = gd.shape[1:]
    wide = pl.BlockSpec((1, rgu, ff), lambda i: (i, 0, 0))
    tall = pl.BlockSpec((1, rd, d), lambda i: (i, 0, 0))
    both = pl.BlockSpec((1, 2, rgu, ff), lambda i: (i, 0, 0, 0))
    specs = [wide, wide, tall] * 3
    size = ggu.size + gd.size
    return pl.pallas_call(
        functools.partial(update_kernel, n * size),
        grid=(layers,),
        out_shape=[jax.ShapeDtypeStruct(a.shape, a.dtype) for a in arrays],
        in_specs=[pl.BlockSpec(memory_space=pltpu.SMEM), both, tall] + specs,
        out_specs=specs,
        compiler_params=pltpu.CompilerParams(vmem_limit_bytes=60 * 2**20),
        cost_estimate=pl.CostEstimate(flops=20 * size, transcendentals=size, bytes_accessed=22 * size),
        name="update",
    )(squares, ggu, gd, *arrays)


def solution(mesh):
    def step(x, dy, *arrays):
        ggu, gd, squares = train(mesh, x[0], dy[0], *arrays[:3])[:3]
        return tuple(update(mesh.shape["dp"], squares, ggu, gd, arrays))

    states, cut = P(("rep", "dp"), None, None), P(None, "dp", None)
    return jax.shard_map(
        step,
        mesh=mesh,
        in_specs=(states, states) + (cut,) * 9,
        out_specs=(P("rep", "dp", None),) * 9,
        check_vma=False,
    )
```
